256 devices in a mesh: groups: 2 (over z), psg: 128 (over x, y, core).
Axes of the slice: x: 8, y: 8, z: 2, core: 2. Of those that a mesh axis runs over, the one named last changes fastest.
The devices are a block of a 8x8x16 slice.
Arguments:
- queries: bfloat16 [512, 32, 128], P(('groups', 'psg')), parts along dimension 0, may hold values from -0.29882812 to 0.29882812
- candidates: int32 [512, 512], P(('groups', 'psg')), parts along dimension 0, may hold values from 0 to 1279
- centroids: bfloat16 [65536, 128], P('psg'), may hold values from -6 to 6
- bucket_weights: float32 [4, 128], replicated, may hold values from -1 to 1
- centroid_shard: int32 [262144, 1], P('psg'), may hold values from 0 to 127; in each aligned block of 2048 rows (0 to 2047, 2048 to 4095, ...) at most 32 rows name the same one
- centroid_row: int32 [262144], P('psg'), may hold values from 0 to 511
- residual_codes: int32 [262144, 128], P('psg'), may hold values from 0 to 3
- tile_count: int32 [1280], replicated, may hold values from 1 to 3, 2048 in all
- last_fill: int32 [1280], replicated, may hold values from 1 to 128
Outputs:
- scores: float32 [512, 512], P(('groups', 'psg')), parts along dimension 0
The draws below stay inside these ranges and needn't reach their ends.
There are 2 independent parts, one for each index of `groups`. The reference program is written for one: setup_inputs(seed, part) draws one part's arguments, and reference() takes and returns one part's arrays. A program takes and returns all parts, laid end to end along the dimension named above; an argument that names none is the same for every part. Nothing has to cross between parts.
Inputs may be any that keep to these rules, and one draw needn't show every extreme that they name: `tile_count`: tiles are numbered along psg, device k holding tiles k * 16 onward; the counts sum to 2048, so a passage may continue on the next device. `centroid_shard`: among the 2048 token slots of one device, at most 32 name the same device; on some device some value is named exactly 32 times.
All inputs are finite; a program needn't handle non-finite values.
Results may differ from the reference program's by a relative error of at most 0.0003.
Values may be sent and summed in bfloat16 or wider, within the bound.
A program may use at most 64 MiB of HBM per device.

```python
import math
import jax
import jax.numpy as jnp
import numpy as np
from jax import lax

DIM = 128
QTOK = 32
TILE = 128
MAXT = 3
CENT_DEV = 512
TILES_DEV = 16
NCAND = 512
CAP = 32
QUERIES = 256
NT = 2048
NP = 1280
NCENT = 65536
TOKENS_ALL = 262144
N_PSG = 128


def with_ends(values, own_key, low, high):
    extent = values.shape
    spot = [jax.random.randint(jax.random.fold_in(own_key, axis), (), 0, extent[axis]) for axis in range(len(extent))]
    values = values.at[tuple(spot)].set(low)
    longest = extent.index(max(extent))
    spot[longest] = (spot[longest] + 1) % extent[longest]
    return values.at[tuple(spot)].set(high)


def shard_levels(rng, shape, cuts, least, top_value):
    def one(dim, parts):
        draws = jax.random.uniform(jax.random.fold_in(jax.random.fold_in(rng, 6), dim), (parts,), jnp.float32, least / len(cuts), top_value / len(cuts))
        return jnp.repeat(jnp.exp(draws), shape[dim] // parts).reshape((-1,) + (1,) * (len(shape) - dim - 1))

    loudness = one(*cuts[0])
    for cut in cuts[1:]:
        loudness = loudness * one(*cut)
    return loudness


def length_profile(number_of, total, bound, slope):
    weights = [(1 << 20) // math.isqrt(grade ** slope) + 1 for grade in range(2, number_of + 1)]
    surplus, holding = total - bound - (number_of - 1), [1] * (number_of - 1)
    while surplus > 0:
        movable = [i for i in range(number_of - 1) if holding[i] < bound]
        mass, budget = sum([weights[i] for i in movable]), surplus
        for i in movable:
            addition = min(bound - holding[i], max(1, budget * weights[i] // mass), surplus)
            holding[i] = holding[i] + addition
            surplus = surplus - addition
    return np.array([bound] + holding)


def ragged_sizes(rng, count, total, bound, slope):
    if count == 2:
        one = jax.random.randint(rng, (), max(1, total - bound), min(bound, total - 1) + 1)
        return jnp.stack([one, total - one])
    lengths = jnp.asarray(length_profile(count, total, bound, slope), jnp.int32)
    twos = (count - 1) // 2
    giver, taker = lengths[1:1 + 2 * twos:2], lengths[2:2 + 2 * twos:2]
    margin = jnp.minimum(giver - 1, bound - taker)
    passed = jax.random.randint(jax.random.fold_in(rng, 1), (twos,), 0, 1 << 20) % (margin + 1)
    lengths = lengths.at[1:1 + 2 * twos:2].set(giver - passed).at[2:2 + 2 * twos:2].set(taker + passed)
    return lengths[jax.random.permutation(jax.random.fold_in(rng, 2), count)]


def routed_block(rng, own, number, rows, count, top, reach, skew):
    ranking = jax.random.permutation(rng, count)
    crowded, common = load_shares(count, rows * top, reach, skew, True), load_shares(count, rows * top, reach, skew, False)
    places = jnp.arange(count)

    def named(sizes, rotation):
        used = int((sizes > 0).sum())
        fixed = max(1, used // 4)
        moved = fixed + (places - fixed + rotation * (used - fixed)) % max(1, count - fixed)
        return jnp.zeros((count,), jnp.int32).at[ranking[jnp.where(places < fixed, places, moved)]].set(jnp.asarray(sizes, jnp.int32))

    sizes = jnp.where(number % 4 == 0, named(crowded, number // 4), named(common, number - number // 4 - 1))
    mixed = jax.random.permutation(jax.random.fold_in(own, 3), count)
    donor, receiver = mixed[0:count // 2 * 2:2], mixed[1:count // 2 * 2:2]
    slack = jnp.minimum(sizes[donor] - 1, reach - sizes[receiver]) // 2
    slack = jnp.where((donor == ranking[0]) | (receiver == ranking[0]) | (sizes[receiver] == 0), 0, jnp.maximum(slack, 0))
    moved = jax.random.randint(jax.random.fold_in(own, 4), (count // 2,), 0, 1 << 20) % (slack + 1)
    sizes = sizes.at[donor].add(-moved).at[receiver].add(moved)
    items = jnp.searchsorted(jnp.cumsum(sizes), jnp.arange(rows * top), side="right").astype(jnp.int32)
    listing = items.reshape(top, rows).T
    listing = listing[jax.random.permutation(jax.random.fold_in(own, 1), rows)]
    rotation = jax.random.randint(jax.random.fold_in(own, 2), (rows, 1), 0, top)
    return jnp.take_along_axis(listing, (jnp.arange(top)[None, :] + rotation) % top, axis=1)


def load_shares(count, total, most, skew, full):
    loads = [(1 << 20) // math.isqrt(rank ** skew) + 1 for rank in range(1, count + 1)]
    largest = most if full else min(most, max(-(-total // count), total * loads[0] // sum(loads)))
    least = 1 if total - largest >= count - 1 else 0
    given, surplus = [largest] + [least] * (count - 1), total - largest - least * (count - 1)
    while surplus > 0:
        movable = [i for i in range(1, count) if given[i] < largest] or [i for i in range(1, count) if given[i] < most]
        pool, budget = sum([loads[i] for i in movable]), surplus
        for i in movable:
            more = min(most - given[i], max(1, budget * loads[i] // pool), surplus)
            given[i] = given[i] + more
            surplus = surplus - more
    return np.array(given)


def gaussian(rng, shape, width, most, split=(), kind=jnp.bfloat16):
    factor_of = shard_levels(rng, shape, split, -0.22, 0.18) if split else 1.0
    result = jax.random.normal(rng, shape, jnp.float32) * width * factor_of
    return jnp.minimum(jnp.maximum(result, -most), most).astype(kind)


def setup_inputs(seed: int = 0, part: int = 0) -> dict:
    keys = jax.random.split(jax.random.key(seed), 10)
    part_keys = jax.random.split(jax.random.fold_in(keys[9], part), 10)
    queries = gaussian(part_keys[0], (QUERIES, QTOK, DIM), 0.05, 0.29882812, ((0, 128),))
    candidates = with_ends(jax.random.randint(part_keys[1], (QUERIES, NCAND), 0, NP), jax.random.fold_in(part_keys[1], 1), 0, NP - 1).astype(jnp.int32)
    centroids = gaussian(keys[2], (NCENT, DIM), 1.0, 6.0, ((0, 128),))
    bucket_weights = jnp.clip(jax.random.uniform(keys[3], (4, DIM), jnp.float32, -1.0, 1.0), -1.0, 1.0)
    centroid_shard_keys = jax.random.split(jax.random.fold_in(keys[4], 1), TOKENS_ALL // (TILES_DEV * TILE))
    centroid_shard_turns = jax.random.permutation(jax.random.fold_in(keys[4], 3), TOKENS_ALL // (TILES_DEV * TILE))
    centroid_shard = jax.vmap(lambda own, number: routed_block(jax.random.fold_in(keys[4], 2), own, number, TILES_DEV * TILE, N_PSG, 1, CAP, 1))(centroid_shard_keys, centroid_shard_turns).reshape((TOKENS_ALL, 1))
    centroid_row = with_ends(jax.random.randint(keys[5], (TOKENS_ALL,), 0, CENT_DEV), jax.random.fold_in(keys[5], 1), 0, CENT_DEV - 1).astype(jnp.int32)
    residual_codes = with_ends(jax.random.randint(keys[6], (TOKENS_ALL, DIM), 0, 4), jax.random.fold_in(keys[6], 1), 0, 3).astype(jnp.int32)
    tile_count = ragged_sizes(keys[7], NP, NT, MAXT, 1).astype(jnp.int32)
    last_fill = with_ends(jax.random.randint(keys[8], (NP,), 1, TILE + 1), jax.random.fold_in(keys[8], 1), 1, TILE).astype(jnp.int32)
    return dict(queries=queries, candidates=candidates, centroids=centroids, bucket_weights=bucket_weights, centroid_shard=centroid_shard, centroid_row=centroid_row, residual_codes=residual_codes, tile_count=tile_count, last_fill=last_fill)


epsilon = 1e-06

def tile_layout(tile_count, last_fill, total_tiles, tile_len):
    starts = (jnp.cumsum(tile_count) - tile_count).astype(jnp.int32)
    last_tile = (starts + tile_count - 1).astype(jnp.int32)
    tile_fill = jnp.full((total_tiles,), tile_len, jnp.int32).at[last_tile].set(last_fill.astype(jnp.int32))
    return (starts, tile_fill)

def decode(picked, residual_codes, bucket_weights):
    residual = jnp.zeros(residual_codes.shape, jnp.float32)
    for bucket in range(4):
        residual = residual + jnp.where(residual_codes == bucket, bucket_weights[bucket][None, :], jnp.float32(0.0))
    summed = picked.astype(jnp.float32) + residual
    scale = lax.rsqrt(lax.optimization_barrier(jnp.sum(summed * summed, axis=1, keepdims=True)) + epsilon)
    return (summed * scale).astype(jnp.bfloat16)

def assemble(own_maxima, candidates, starts, tile_count, query_len):
    num_queries, num_cand = candidates.shape
    own_maxima = own_maxima.reshape(num_queries, query_len, -1)
    tile_steps = jnp.arange(MAXT, dtype=jnp.int32)
    tile_index = starts[candidates][..., None] + tile_steps
    live_mask = tile_steps < tile_count[candidates][..., None]
    tile_index = jnp.where(live_mask, tile_index, 0).astype(jnp.int32)
    values = jax.vmap(lambda matrix, indices: matrix[:, indices.reshape(-1)])(own_maxima, tile_index)
    values = values.reshape(num_queries, query_len, num_cand, MAXT)
    values = jnp.where(live_mask[:, None], values, -jnp.inf)
    return lax.optimization_barrier(jnp.sum(lax.optimization_barrier(jnp.max(values, axis=3)), axis=1))

def reference(queries, candidates, centroids, bucket_weights, centroid_shard, centroid_row, residual_codes, tile_count, last_fill):
    total_tiles = TILES_DEV * N_PSG
    starts, tile_fill = tile_layout(tile_count, last_fill, total_tiles, TILE)
    codes = (centroid_shard[:, 0] * CENT_DEV + centroid_row).astype(jnp.int32)
    picked = jnp.take(centroids, codes, axis=0)
    embedded = decode(picked, residual_codes, bucket_weights)
    token_mask = jnp.arange(TILE, dtype=jnp.int32)[None, :] < tile_fill[:, None]
    pad_bias = jnp.where(token_mask, jnp.float32(0.0), -jnp.inf).reshape(N_PSG, TILES_DEV * TILE)
    key_blocks = embedded.reshape(N_PSG, TILES_DEV * TILE, DIM)
    flat_rows = queries.reshape(-1, DIM)

    def one_block(inputs):
        key_block, bias_block = inputs
        block_scores = jnp.dot(flat_rows, key_block.T, preferred_element_type=jnp.float32) + bias_block[None, :]
        return lax.optimization_barrier(jnp.max(block_scores.reshape(flat_rows.shape[0], TILES_DEV, TILE), axis=2))
    maxima = lax.map(one_block, (key_blocks, pad_bias))
    maxima = jnp.transpose(maxima, (1, 0, 2)).reshape(flat_rows.shape[0], total_tiles)
    return assemble(maxima, candidates, starts, tile_count, QTOK)
```

```python
import jax
import jax.numpy as jnp
from jax import lax
from jax.experimental import pallas as pl
from jax.experimental.pallas import tpu as pltpu
from jax.sharding import Mesh
from jax.sharding import PartitionSpec as P

TILE = 128
PSG = ("psg_0", "psg_1", "psg_2")
GROUPS_PSG = ("groups", "psg_0", "psg_1", "psg_2")


epsilon = 1e-06


def split_up(shard, dim, length):
    shape = shard.shape
    blocks = shard.reshape(*shape[:dim], length, shape[dim] // length, *shape[dim + 1 :])
    return jnp.moveaxis(blocks, dim, 0)


def joined_along(blocks, dim):
    blocks = jnp.moveaxis(blocks, 0, dim)
    shape = blocks.shape
    return blocks.reshape(*shape[:dim], shape[dim] * shape[dim + 1], *shape[dim + 2 :])


def exchange_in_order(blocks, axes, order):
    shape = [lax.axis_size(a) for a in axes]
    blocks = blocks.reshape(*shape, *blocks.shape[1:])
    for k in order:
        blocks = lax.all_to_all(blocks, axes[k], split_axis=k, concat_axis=k, tiled=True)
    return blocks.reshape(-1, *blocks.shape[len(axes) :])


def two_step_exchange(shard, groups, order, split_dim, concat_dim):
    length = lax.axis_size(groups[0]) * lax.axis_size(groups[1])
    blocks = split_up(shard, split_dim, length)
    return joined_along(exchange_in_order(blocks, groups, order), concat_dim)


MESH = pl.DeviceIdType.MESH
OFFSETS = tuple(
    (a, (a + b) % 8, c)
    for b in range(8)
    for a in range(8)
    for c in range(2)
    if (a, (a + b) % 8, c) != (0, 0, 0)
)


def exchange_kernel(rows, src, dst, send_sem, recv_sem, own_sem):
    x, y, c = (lax.axis_index(name) for name in PSG)
    xs = [lax.rem(x + d, 8) for d in range(8)]
    ys = [lax.rem(y + d, 8) for d in range(8)]
    cs = [c, 1 - c]
    barrier = pltpu.get_barrier_semaphore()
    for i, j, k in OFFSETS:
        pl.semaphore_signal(
            barrier,
            inc=1,
            device_id={"psg_0": xs[i], "psg_1": ys[j], "psg_2": cs[k]},
            device_id_type=MESH,
        )
    pl.semaphore_wait(barrier, len(OFFSETS))
    me = pl.multiple_of((x * 16 + y * 2 + c) * rows, rows)
    own = pltpu.make_async_copy(src.at[pl.ds(me, rows)], dst.at[pl.ds(me, rows)], own_sem)
    own.start()
    for i, j, k in OFFSETS:
        peer = pl.multiple_of((xs[i] * 16 + ys[j] * 2 + cs[k]) * rows, rows)
        pltpu.make_async_remote_copy(
            src_ref=src.at[pl.ds(peer, rows)],
            dst_ref=dst.at[pl.ds(me, rows)],
            send_sem=send_sem,
            recv_sem=recv_sem,
            device_id={"psg_0": xs[i], "psg_1": ys[j], "psg_2": cs[k]},
            device_id_type=MESH,
        ).start()
    own.wait()
    rest = pl.ds(0, len(OFFSETS) * rows)
    pltpu.make_async_copy(src.at[rest], dst.at[rest], send_sem).wait()
    pltpu.make_async_copy(src.at[rest], dst.at[rest], recv_sem).wait()


def exchange(array, number):
    rows = array.shape[0] // 128
    import functools

    return pl.pallas_call(
        functools.partial(exchange_kernel, rows),
        out_shape=jax.ShapeDtypeStruct(array.shape, array.dtype),
        in_specs=[pl.BlockSpec(memory_space=pl.ANY)],
        out_specs=pl.BlockSpec(memory_space=pl.ANY),
        scratch_shapes=[pltpu.SemaphoreType.DMA] * 3,
        compiler_params=pltpu.CompilerParams(collective_id=number, has_side_effects=True),
    )(array)


def tile_layout(tile_count, last_fill, total_tiles, tile_len):
    starts = jnp.cumsum(tile_count) - tile_count
    last_tile = starts + tile_count - 1
    tile_fill = jnp.full((total_tiles,), tile_len, jnp.int32).at[last_tile].set(last_fill)
    return (starts, tile_fill)


def decode(picked, residual_codes, bucket_weights):
    residual = jnp.zeros(residual_codes.shape, jnp.float32)
    for bucket in range(4):
        residual = residual + jnp.where(
            residual_codes == bucket, bucket_weights[bucket][None, :], jnp.float32(0.0)
        )
    summed = picked.astype(jnp.float32) + residual
    scale = lax.rsqrt(jnp.sum(summed * summed, axis=1, keepdims=True) + epsilon)
    return (summed * scale).astype(jnp.bfloat16)


def assemble(own_maxima, candidates, starts, total_tiles, query_len):
    num_queries, num_cand = candidates.shape
    marker = jnp.zeros((total_tiles,), jnp.int32).at[starts].add(1)
    owner_id = jnp.cumsum(marker)
    same_next = jnp.concatenate([owner_id[1:] == owner_id[:-1], jnp.zeros((1,), bool)])
    same_after = jnp.concatenate([owner_id[2:] == owner_id[:-2], jnp.zeros((2,), bool)])
    shifted_one = jnp.concatenate([own_maxima[:, 1:], own_maxima[:, :1]], axis=1)
    shifted_two = jnp.concatenate([own_maxima[:, 2:], own_maxima[:, :2]], axis=1)
    combined = jnp.maximum(own_maxima, jnp.where(same_next[None, :], shifted_one, own_maxima))
    combined = jnp.maximum(combined, jnp.where(same_after[None, :], shifted_two, own_maxima))
    combined = combined.reshape(num_queries, query_len, total_tiles)
    first_tile = starts[candidates]
    selector = (
        first_tile[:, :, None] == jnp.arange(total_tiles, dtype=jnp.int32)[None, None, :]
    ).astype(jnp.float32)
    return jnp.einsum(
        "qit,qct->qc",
        combined,
        selector,
        precision=lax.Precision.HIGHEST,
        preferred_element_type=jnp.float32,
    )


def per_device(
    queries,
    candidates,
    centroids,
    bucket_weights,
    centroid_shard,
    centroid_row,
    residual_codes,
    tile_count,
    last_fill,
):
    n_psg = lax.axis_size(PSG)
    shard_index = lax.axis_index(PSG)
    tok_dev = residual_codes.shape[0]
    tiles_dev = tok_dev // TILE
    owners = centroid_shard[:, 0]
    capacity = max(2, 2 * tok_dev // n_psg)
    onehot = (owners[:, None] == jnp.arange(n_psg, dtype=jnp.int32)[None, :]).astype(jnp.int32)
    rank_in = jnp.sum((jnp.cumsum(onehot, axis=0) - 1) * onehot, axis=1)
    slot_of = owners * capacity + rank_in
    requests = (
        jnp.zeros((n_psg * capacity,), jnp.int32)
        .at[slot_of]
        .set(centroid_row)
        .reshape(n_psg, capacity)
    )
    wide = jnp.zeros((n_psg, 8, 128), jnp.int32).at[:, 0, :capacity].set(requests)
    asked = exchange(wide.reshape(n_psg * 8, 128), 0).reshape(n_psg, 8, 128)[:, 0, :capacity]
    found = jnp.take(centroids, asked, axis=0)
    fetched = exchange(found.reshape(n_psg * capacity, -1), 1)
    picked = jnp.take(fetched.reshape(n_psg * capacity, -1), slot_of, axis=0)
    embedded = decode(picked, residual_codes, bucket_weights)
    total_tiles = tiles_dev * n_psg
    starts, tile_fill = tile_layout(tile_count, last_fill, total_tiles, TILE)
    local_fill = lax.dynamic_slice_in_dim(tile_fill, shard_index * tiles_dev, tiles_dev, 0)
    token_mask = jnp.arange(TILE, dtype=jnp.int32)[None, :] < local_fill[:, None]
    pad_bias = jnp.where(token_mask, jnp.float32(0.0), -jnp.inf).reshape(-1)
    per_block = max(1, 512 // TILE)
    while tiles_dev % per_block:
        per_block -= 1
    width = per_block * TILE
    piece = lax.all_gather(queries, PSG, axis=0, tiled=True)
    flat_rows = piece.reshape(-1, piece.shape[-1])
    pieces = []
    for block in range(tiles_dev // per_block):
        key_block = embedded[block * width : (block + 1) * width]
        block_scores = jnp.einsum(
            "qd,kd->qk", flat_rows, key_block, preferred_element_type=jnp.float32
        )
        block_scores = block_scores + pad_bias[block * width : (block + 1) * width][None, :]
        pieces.append(jnp.max(block_scores.reshape(flat_rows.shape[0], per_block, TILE), axis=2))
    maxima = jnp.concatenate(pieces, axis=1)
    own_maxima = lax.all_to_all(maxima, PSG, split_axis=0, concat_axis=1, tiled=True)
    return assemble(own_maxima, candidates, starts, total_tiles, queries.shape[1])


def solution(mesh):
    torus = Mesh(
        mesh.devices.reshape(mesh.shape["groups"], 8, 8, 2), ("groups", "psg_0", "psg_1", "psg_2")
    )
    return jax.shard_map(
        per_device,
        mesh=torus,
        in_specs=(
            P(GROUPS_PSG, None, None),
            P(GROUPS_PSG, None),
            P(PSG, None),
            P(),
            P(PSG, None),
            P(PSG),
            P(PSG, None),
            P(),
            P(),
        ),
        out_specs=P(GROUPS_PSG, None),
        check_vma=False,
    )
```

```python
import functools

import jax
import jax.numpy as jnp
from jax import lax
from jax.experimental import pallas as pl
from jax.experimental.pallas import tpu as pltpu
from jax.sharding import PartitionSpec as P

MESH = pl.DeviceIdType.MESH
TILE = 128
LANES = 128
NX, NY, NC = 8, 8, 2
CAP = 32
EPS = 1e-06
F32, BF16, I32 = jnp.float32, jnp.bfloat16, jnp.int32


def dot(a, b, ca=1, cb=0):
    return lax.dot_general(a, b, (((ca,), (cb,)), ((), ())), preferred_element_type=F32)


def kernel(
    owner_ref,
    row_ref,
    cent_hbm,
    code_hbm,
    bw_ref,
    count_ref,
    last_ref,
    query_ref,
    cand_ref,
    out_ref,
    cent,
    code,
    req,
    asked,
    onehot,
    sent,
    fetched,
    low,
    high,
    res,
    acc,
    emb,
    qb,
    tm,
    head_out,
    head_in,
    wide,
    got,
    starts,
    fills,
    join1,
    join2,
    load_sem,
    req_send,
    req_recv,
    row_send,
    row_recv,
    qx_send,
    qx_recv,
    qup_send,
    qup_recv,
    qdn_send,
    qdn_recv,
    qc_send,
    qc_recv,
    head_send,
    head_recv,
    score_send,
    score_recv,
):
    n = NX * NY * NC
    tiles = owner_ref.shape[0]
    npass = count_ref.shape[0]
    me = lax.axis_index("psg")
    x = me // (NY * NC)
    y = lax.rem(me // NC, NY)
    c = lax.rem(me, NC)
    other = 1 - c

    def index(px, py, pc):
        return (px * NY + py) * NC + pc

    def ahead(g, a, k):
        px, py = lax.rem(x + a, NX), lax.rem(y + a + g, NY)
        return px, py, index(px, py, c if k == 0 else other)

    def behind(g, a, k):
        px, py = lax.rem(x + NX - a, NX), lax.rem(y + 2 * NY - a - g, NY)
        return index(px, py, c if k == 0 else other)

    def relative(device):
        dx = (x - device // (NY * NC)) & (NX - 1)
        dy = (y - (device // NC) % NY) & (NY - 1)
        dc = (c - device) & (NC - 1)
        return ((dy - dx) & (NY - 1)) * (NX * NC) + dx * NC + dc

    pairs = [(a, k) for a in range(NX) for k in range(NC)]
    group = NX * NC
    gslots = group * CAP

    barrier = pltpu.get_barrier_semaphore()
    for g in range(NY):
        for a, k in pairs:
            if (g, a, k) != (0, 0, 0):
                pl.semaphore_signal(
                    barrier, inc=1, device_id={"psg": ahead(g, a, k)[2]}, device_id_type=MESH
                )
    cent_copy = pltpu.make_async_copy(cent_hbm, cent, load_sem.at[0])
    cent_copy.start()
    code_copy = pltpu.make_async_copy(code_hbm, code, load_sem.at[1])
    code_copy.start()

    sub = lax.broadcasted_iota(I32, (LANES, LANES), 0)
    lane = lax.broadcasted_iota(I32, (LANES, LANES), 1)
    upper = (sub <= lane).astype(BF16)
    ones = jnp.ones((LANES, LANES), BF16)
    rel = relative(owner_ref[...])
    crow = row_ref[...]
    carry = jnp.zeros((LANES, LANES), F32)
    low_sum = jnp.zeros((LANES, LANES), F32)
    high_sum = jnp.zeros((LANES, LANES), F32)
    slots = []
    for t in range(tiles):
        member = sub == rel[t : t + 1, :]
        flags = member.astype(BF16)
        running = dot(flags, upper) + carry
        carry = carry + dot(flags, ones)
        rank = jnp.sum(jnp.where(member, running, 0.0), axis=0, keepdims=True).astype(I32) - 1
        slots.append(rel[t : t + 1, :] * CAP + rank)
        place = sub == rank
        tok = crow[t : t + 1, :]
        low_sum = low_sum + dot(
            flags, jnp.where(place, (tok & 255).astype(F32), 0.0).astype(BF16), 1, 1
        )
        high_sum = high_sum + dot(
            flags, jnp.where(place, (tok >> 8).astype(F32), 0.0).astype(BF16), 1, 1
        )
    req[...] = (low_sum + 256.0 * high_sum).astype(I32)

    pl.semaphore_wait(barrier, n - 1)
    asked[0:1, :] = req[0:1, :]
    for g in range(NY):
        for a, k in pairs:
            if (g, a, k) != (0, 0, 0):
                j = g * group + a * NC + k
                pltpu.make_async_remote_copy(
                    src_ref=req.at[pl.ds(j, 1)],
                    dst_ref=asked.at[pl.ds(j, 1)],
                    send_sem=req_send,
                    recv_sem=req_recv.at[g],
                    device_id={"psg": behind(g, a, k)},
                    device_id_type=MESH,
                ).start()

    nq = query_ref.shape[0]
    for a in range(1, NX):
        px = lax.rem(x + a, NX)
        pltpu.make_async_remote_copy(
            src_ref=query_ref,
            dst_ref=qb.at[y, c, pl.ds(pl.multiple_of(x * nq, nq), nq)],
            send_sem=qx_send,
            recv_sem=qx_recv,
            device_id={"psg": index(px, y, c)},
            device_id_type=MESH,
        ).start()
    qb[y, c, pl.ds(pl.multiple_of(x * nq, nq), nq), :] = query_ref[...]

    slot = jnp.concatenate(slots, axis=0)
    pad = jnp.zeros((LANES - tiles, LANES), F32)
    low_t = jnp.concatenate([(slot & 255).astype(F32), pad], axis=0).T
    high_t = jnp.concatenate([(slot >> 8).astype(F32), pad], axis=0).T
    wide_lane = lax.broadcasted_iota(I32, (LANES, 256), 1).astype(F32)
    for t in range(tiles):
        at = pl.ds(t * TILE, TILE)
        low[at, :] = (low_t[:, t : t + 1] == wide_lane).astype(BF16)
        high[at, :] = jnp.broadcast_to(high_t[:, t : t + 1], (TILE, LANES))

    counts = count_ref[...].astype(F32)
    sums = dot(counts.astype(BF16), upper)
    before = jnp.zeros((1, 1), F32)
    rows = []
    for r in range(npass):
        rows.append(sums[r : r + 1, :] + before)
        before = before + sums[r : r + 1, LANES - 1 : LANES]
    ends = jnp.concatenate(rows, axis=0)
    starts[...] = (ends - counts).astype(I32)
    final = ends.astype(I32) - 1
    last = last_ref[...].astype(F32)
    fill_rows, end_rows = [], []
    for t in range(tiles + 1):
        hit = final == me * tiles + t
        fill_rows.append(jnp.sum(jnp.where(hit, last, 0.0), axis=0, keepdims=True))
        end_rows.append(jnp.sum(jnp.where(hit, 1.0, 0.0), axis=0, keepdims=True))
    fill = jnp.sum(jnp.concatenate(fill_rows, axis=0), axis=1, keepdims=True)
    ending = jnp.sum(jnp.concatenate(end_rows, axis=0), axis=1, keepdims=True)
    fills[...] = jnp.broadcast_to(jnp.where(ending > 0, fill, float(TILE))[:tiles], (tiles, LANES))
    goes = ending == 0
    join1[...] = jnp.broadcast_to(goes[:tiles].astype(F32), (tiles, LANES))
    join2[...] = jnp.broadcast_to(
        goes[:tiles].astype(F32) * goes[1 : tiles + 1].astype(F32), (tiles, LANES)
    )

    up = index(x, lax.rem(y + 1, NY), c)
    down = index(x, lax.rem(y + NY - 1, NY), c)
    across = index(x, y, other)
    n_up, n_down = NY // 2, NY - 1 - NY // 2

    def pass_on(block, where, send, recv):
        pltpu.make_async_remote_copy(
            src_ref=qb.at[block, c],
            dst_ref=qb.at[block, c],
            send_sem=send,
            recv_sem=recv,
            device_id={"psg": where},
            device_id_type=MESH,
        ).start()

    def arrived(ref, sem):
        pltpu.make_async_copy(ref, ref, sem).wait()

    arrived(qb.at[y, c, pl.ds(0, (NX - 1) * nq)], qx_recv)
    pass_on(y, up, qup_send, qup_recv.at[0])
    pass_on(y, down, qdn_send, qdn_recv.at[0])
    pass_on(y, across, qc_send, qc_recv)

    cent_copy.wait()
    half_lane = lax.broadcasted_iota(I32, (CAP, cent.shape[0]), 1).astype(F32)

    def ring(s):
        block = lax.rem(y + NY - s, NY)
        arrived(qb.at[block, c], qup_recv.at[s - 1])
        if s < n_up:
            pass_on(block, up, qup_send, qup_recv.at[s])
        pass_on(block, across, qc_send, qc_recv)
        if s <= n_down:
            block = lax.rem(y + s, NY)
            arrived(qb.at[block, c], qdn_recv.at[s - 1])
            if s < n_down:
                pass_on(block, down, qdn_send, qdn_recv.at[s])
            pass_on(block, across, qc_send, qc_recv)

    for g in range(NY):
        count = group - 1 if g == 0 else group
        arrived(asked.at[pl.ds(0, count)], req_recv.at[g])
        wanted = asked[pl.ds(g * group, group), :].astype(F32).T
        for j in range(group):
            onehot[pl.ds(j * CAP, CAP), :] = (wanted[:CAP, j : j + 1] == half_lane).astype(BF16)
        found = dot(onehot[...], cent[...]).astype(BF16)
        sent[pl.ds(g * gslots, gslots), :] = found
        if g == 0:
            fetched[pl.ds(0, CAP), :] = found[:CAP]
        for a, k in pairs:
            if (g, a, k) != (0, 0, 0):
                at = pl.ds((g * group + a * NC + k) * CAP, CAP)
                pltpu.make_async_remote_copy(
                    src_ref=sent.at[at],
                    dst_ref=fetched.at[at],
                    send_sem=row_send,
                    recv_sem=row_recv.at[g],
                    device_id={"psg": ahead(g, a, k)[2]},
                    device_id_type=MESH,
                ).start()
        if g % 2 == 0:
            ring(g // 2 + 1)

    code_copy.wait()

    @pl.loop(0, tiles)
    def _(t):
        at = pl.ds(pl.multiple_of(t * TILE, TILE), TILE)
        v = code[at, :]
        first = jnp.where(v == 0, bw_ref[0:1, :], bw_ref[1:2, :])
        second = jnp.where(v == 2, bw_ref[2:3, :], bw_ref[3:4, :])
        res[at, :] = jnp.where(v < 2, first, second)

    span = 4 * TILE
    for g in range(NY):
        count = (group - 1 if g == 0 else group) * CAP
        arrived(fetched.at[pl.ds(0, count)], row_recv.at[g])
        base = g * gslots
        both = jnp.concatenate(
            [fetched[pl.ds(base, 256), :], fetched[pl.ds(base + 256, 256), :]], axis=1
        )

        @pl.loop(0, tiles * TILE // span)
        def _(i):
            at = pl.ds(pl.multiple_of(i * span, span), span)
            picked = dot(low[at, :], both)
            which = high[at, :]
            keep = 0.0 if g == 0 else acc[at, :]
            keep = jnp.where(which == float(2 * g + 1), picked[:, LANES:], keep)
            acc[at, :] = jnp.where(which == float(2 * g), picked[:, :LANES], keep)

    @pl.loop(0, tiles)
    def _(t):
        at = pl.ds(pl.multiple_of(t * TILE, TILE), TILE)
        summed = acc[at, :] + res[at, :]
        scale = lax.rsqrt(jnp.sum(summed * summed, axis=1, keepdims=True) + EPS)
        unit = summed * scale
        unit = jnp.where(sub.astype(F32) < fills[pl.ds(t, 1), :], unit, unit[0:1, :])
        emb[at, :] = unit.astype(BF16)

    arrived(qb.at[pl.ds(0, NY), 0], qc_recv)

    span = tiles // 2
    chunk = 256
    per = qb.shape[2] // chunk

    def maxima(half):
        @pl.loop(0, NY * NC * per)
        def _(i):
            part = qb[
                i // (NC * per),
                lax.rem(i // per, NC),
                pl.ds(pl.multiple_of(lax.rem(i, per) * chunk, chunk), chunk),
                :,
            ]
            at = pl.ds(pl.multiple_of(i * chunk, chunk), chunk)
            s = dot(emb[pl.ds(half * span * TILE, span * TILE), :], part, 1, 1)
            top = jnp.max(s.reshape(span, TILE, chunk), axis=1)
            tm[pl.ds(half * span, span), at] = top
            if half == 0:
                head_out[:, at] = top[0:2, :]

    maxima(0)
    pltpu.make_async_remote_copy(
        src_ref=head_out,
        dst_ref=head_in,
        send_sem=head_send,
        recv_sem=head_recv,
        device_id={"psg": lax.rem(me + n - 1, n)},
        device_id_type=MESH,
    ).start()
    maxima(1)
    arrived(head_in, head_recv)
    tm[tiles : tiles + 2, :] = head_in[...]

    width = NX * LANES
    first_join, second_join = join1[...] > 0, join2[...] > 0
    for b in range(NY):
        stack = []
        for i in range(NX):
            at = pl.ds(b * width + i * LANES, LANES)
            one = tm[0:tiles, at]
            one = jnp.maximum(one, jnp.where(first_join, tm[1 : tiles + 1, at], one))
            one = jnp.maximum(one, jnp.where(second_join, tm[2 : tiles + 2, at], one))
            stack.append(one)
        turned = jnp.concatenate(stack, axis=0).T
        total = jnp.sum(turned.reshape(4, 32, LANES), axis=1)
        wide[2 * b] = total[0:2]
        wide[2 * b + 1] = total[2:4]

    for g in range(NY):
        for a, k in pairs:
            j = g * group + a * NC + k
            if j == 0:
                got[0] = wide[y * 2 + lax.rem(x, 2)]
                continue
            px, py, peer = ahead(g, a, k)
            pltpu.make_async_remote_copy(
                src_ref=wide.at[py * 2 + lax.rem(px, 2)],
                dst_ref=got.at[j],
                send_sem=score_send,
                recv_sem=score_recv,
                device_id={"psg": peer},
                device_id_type=MESH,
            ).start()

    cand = cand_ref[...]
    tile = jnp.zeros(cand.shape, I32)
    for r in range(npass):
        table = jnp.broadcast_to(starts[r : r + 1, :], cand.shape)
        value = jnp.take_along_axis(table, cand & (LANES - 1), axis=1)
        tile = jnp.where(cand >> 7 == r, value, tile)
    source, slot_of = relative(tile // tiles), tile % tiles
    upper_half = lax.broadcasted_iota(I32, cand.shape, 0) < cand.shape[0] // 2
    turn = lax.rem(LANES - (c * (NX // 2) + x // 2) * tiles, LANES)

    arrived(got.at[pl.ds(0, n - 1)], score_recv)
    tables = [pltpu.roll(got[:, i, :], turn, 1).T for i in range(2)]
    score = jnp.zeros(cand.shape, F32)
    for s in range(tiles):
        table = jnp.where(upper_half, tables[0][s : s + 1, :], tables[1][s : s + 1, :])
        value = jnp.take_along_axis(table, source, axis=1)
        score = jnp.where(slot_of == s, value, score)
    out_ref[...] = score

    arrived(req.at[pl.ds(0, n - 1)], req_send)
    arrived(sent.at[pl.ds(0, (n - 1) * CAP)], row_send)
    arrived(qb.at[0, 0, pl.ds(0, (NX - 1) * nq)], qx_send)
    arrived(qb.at[pl.ds(0, n_up), 0], qup_send)
    arrived(qb.at[pl.ds(0, n_down), 0], qdn_send)
    arrived(qb.at[pl.ds(0, NY), 0], qc_send)
    arrived(head_out, head_send)
    arrived(got.at[pl.ds(0, n - 1)], score_send)


def per_device(
    queries,
    candidates,
    centroids,
    bucket_weights,
    centroid_shard,
    centroid_row,
    residual_codes,
    tile_count,
    last_fill,
):
    n = NX * NY * NC
    tok, dim = residual_codes.shape
    tiles = tok // TILE
    nq = queries.shape[0] * queries.shape[1]
    ncand = candidates.size // LANES
    npass = tile_count.shape[0] // LANES
    dma = pltpu.SemaphoreType.DMA
    vmem = pl.BlockSpec(memory_space=pltpu.VMEM)
    anywhere = pl.BlockSpec(memory_space=pl.ANY)
    score = pl.pallas_call(
        kernel,
        out_shape=jax.ShapeDtypeStruct((ncand, LANES), F32),
        in_specs=[vmem, vmem, anywhere, anywhere, vmem, vmem, vmem, vmem, vmem],
        out_specs=vmem,
        scratch_shapes=[
            pltpu.VMEM(centroids.shape, BF16),
            pltpu.VMEM(residual_codes.shape, I32),
            pltpu.VMEM((n, LANES), I32),
            pltpu.VMEM((n, LANES), I32),
            pltpu.VMEM((NX * NC * CAP, centroids.shape[0]), BF16),
            pltpu.VMEM((n * CAP, dim), BF16),
            pltpu.VMEM((n * CAP, dim), BF16),
            pltpu.VMEM((tok, 256), BF16),
            pltpu.VMEM((tok, LANES), F32),
            pltpu.VMEM((tok, dim), F32),
            pltpu.VMEM((tok, dim), F32),
            pltpu.VMEM((tok, dim), BF16),
            pltpu.VMEM((NY, NC, NX * nq, dim), BF16),
            pltpu.VMEM((tiles + 8, n * nq), F32),
            pltpu.VMEM((2, n * nq), F32),
            pltpu.VMEM((2, n * nq), F32),
            pltpu.VMEM((2 * NY, 2, LANES), F32),
            pltpu.VMEM((n, 2, LANES), F32),
            pltpu.VMEM((npass, LANES), I32),
            pltpu.VMEM((tiles, LANES), F32),
            pltpu.VMEM((tiles, LANES), F32),
            pltpu.VMEM((tiles, LANES), F32),
            dma((2,)),
            dma,
            dma((NY,)),
            dma,
            dma((NY,)),
            dma,
            dma,
            dma,
            dma((NY // 2,)),
            dma,
            dma((NY // 2,)),
            dma,
            dma,
            dma,
            dma,
            dma,
            dma,
        ],
        compiler_params=pltpu.CompilerParams(collective_id=0, has_side_effects=True),
    )(
        centroid_shard.reshape(tiles, TILE),
        centroid_row.reshape(tiles, TILE),
        centroids,
        residual_codes,
        bucket_weights,
        tile_count.reshape(npass, LANES),
        last_fill.reshape(npass, LANES),
        queries.reshape(nq, dim),
        candidates.reshape(ncand, LANES),
    )
    return score.reshape(candidates.shape)


def solution(mesh):
    both = ("groups", "psg")
    return jax.shard_map(
        per_device,
        mesh=mesh,
        in_specs=(
            P(both, None, None),
            P(both, None),
            P("psg", None),
            P(),
            P("psg", None),
            P("psg"),
            P("psg", None),
            P(),
            P(),
        ),
        out_specs=P(both, None),
        check_vma=False,
    )
```

```python
import functools

import jax
import jax.numpy as jnp
from jax import lax
from jax.experimental import pallas as pl
from jax.experimental.pallas import tpu as pltpu
from jax.sharding import PartitionSpec as P

MESH = pl.DeviceIdType.MESH
TILE = 128
LANES = 128
NX, NY, NC = 8, 8, 2
CAP = 32
EPS = 1e-06
F32, BF16, I32 = jnp.float32, jnp.bfloat16, jnp.int32


def dot(a, b, ca=1, cb=0):
    return lax.dot_general(a, b, (((ca,), (cb,)), ((), ())), preferred_element_type=F32)


def kernel(
    owner_ref,
    row_ref,
    cent_hbm,
    code_hbm,
    bw_ref,
    count_ref,
    last_ref,
    query_ref,
    cand_ref,
    out_ref,
    cent,
    code,
    req,
    mid_req,
    asked,
    onehot,
    sent,
    fetched,
    low,
    high,
    res,
    acc,
    emb,
    qb,
    tm,
    head_out,
    head_in,
    wide,
    mid,
    got,
    starts,
    fills,
    join1,
    join2,
    load_sem,
    rx_send,
    rx_recv,
    ry_send,
    ry_recv,
    row_send,
    row_recv,
    qx_send,
    qx_recv,
    qup_send,
    qup_recv,
    qdn_send,
    qdn_recv,
    qc_send,
    qc_recv,
    head_send,
    head_recv,
    s1_send,
    s1_recv,
    s2_send,
    s2_recv,
):
    n = NX * NY * NC
    tiles = owner_ref.shape[0]
    npass = count_ref.shape[0]
    me = lax.axis_index("psg")
    x = me // (NY * NC)
    y = lax.rem(me // NC, NY)
    c = lax.rem(me, NC)
    other = 1 - c

    def index(px, py, pc):
        return (px * NY + py) * NC + pc

    def ahead(g, a, k):
        px, py = lax.rem(x + a, NX), lax.rem(y + a + g, NY)
        return px, py, index(px, py, c if k == 0 else other)

    def shift(device):
        dx = (x - device // (NY * NC)) & (NX - 1)
        dy = (y - (device // NC) % NY) & (NY - 1)
        dc = (c - device) & (NC - 1)
        return dx, dy, dc

    def push(src, dst, where, send, recv):
        pltpu.make_async_remote_copy(
            src_ref=src,
            dst_ref=dst,
            send_sem=send,
            recv_sem=recv,
            device_id={"psg": where},
            device_id_type=MESH,
        ).start()

    def arrived(ref, sem):
        pltpu.make_async_copy(ref, ref, sem).wait()

    def at_uv(u, v):
        return (1 - c) * index(v, u, 0) + c * index(u, v, 1)

    u, v = y + c * (x - y), x + c * (y - x)

    pairs = [(a, k) for a in range(NX) for k in range(NC)]
    group = NX * NC
    gslots = group * CAP

    barrier = pltpu.get_barrier_semaphore()
    for g in range(NY):
        for a, k in pairs:
            if (g, a, k) != (0, 0, 0):
                pl.semaphore_signal(
                    barrier, inc=1, device_id={"psg": ahead(g, a, k)[2]}, device_id_type=MESH
                )
    cent_copy = pltpu.make_async_copy(cent_hbm, cent, load_sem.at[0])
    cent_copy.start()
    code_copy = pltpu.make_async_copy(code_hbm, code, load_sem.at[1])
    code_copy.start()

    sub = lax.broadcasted_iota(I32, (LANES, LANES), 0)
    lane = lax.broadcasted_iota(I32, (LANES, LANES), 1)
    upper = (sub <= lane).astype(BF16)
    ones = jnp.ones((LANES, LANES), BF16)
    dx, dy, dc = shift(owner_ref[...])
    rel = (dx * NY + dy) * NC + dc
    turn_of = ((dy - dx) & (NY - 1)) * (NX * NC) + dx * NC + dc
    crow = row_ref[...]
    carry = jnp.zeros((LANES, LANES), F32)
    low_sum = jnp.zeros((LANES, LANES), F32)
    high_sum = jnp.zeros((LANES, LANES), F32)
    slots = []
    for t in range(tiles):
        member = sub == rel[t : t + 1, :]
        flags = member.astype(BF16)
        running = dot(flags, upper) + carry
        carry = carry + dot(flags, ones)
        rank = jnp.sum(jnp.where(member, running, 0.0), axis=0, keepdims=True).astype(I32) - 1
        slots.append(turn_of[t : t + 1, :] * CAP + rank)
        place = sub == rank
        tok = crow[t : t + 1, :]
        low_sum = low_sum + dot(
            flags, jnp.where(place, (tok & 255).astype(F32), 0.0).astype(BF16), 1, 1
        )
        high_sum = high_sum + dot(
            flags, jnp.where(place, (tok >> 8).astype(F32), 0.0).astype(BF16), 1, 1
        )
    asking = (low_sum + 256.0 * high_sum).astype(I32)
    req[...] = asking.reshape(NX, NY * NC, LANES)

    pl.semaphore_wait(barrier, n - 1)

    for a in range(1, NX):
        where = index(lax.rem(x + NX - a, NX), y, c)
        push(req.at[a], mid_req.at[a], where, rx_send, rx_recv)
    mid_req[0] = req[0]

    nq = query_ref.shape[0]
    own_block = qb.at[u, c, pl.ds(pl.multiple_of(v * nq, nq), nq)]
    for a in range(1, NX):
        push(query_ref, own_block, at_uv(u, lax.rem(v + a, NX)), qx_send, qx_recv)
    qb[u, c, pl.ds(pl.multiple_of(v * nq, nq), nq), :] = query_ref[...]

    arrived(mid_req.at[pl.ds(0, NX - 1)], rx_recv)
    for j in range(1, NY * NC):
        d, k = j // NC, j % NC
        where = index(x, lax.rem(y + NY - d, NY), c if k == 0 else other)
        push(mid_req.at[:, j], asked.at[j], where, ry_send, ry_recv)
    asked[0] = mid_req[:, 0, :]

    slot = jnp.concatenate(slots, axis=0)
    pad = jnp.zeros((LANES - tiles, LANES), F32)
    low_t = jnp.concatenate([(slot & 255).astype(F32), pad], axis=0).T
    high_t = jnp.concatenate([(slot >> 8).astype(F32), pad], axis=0).T
    wide_lane = lax.broadcasted_iota(I32, (LANES, 256), 1).astype(F32)
    for t in range(tiles):
        at = pl.ds(t * TILE, TILE)
        low[at, :] = (low_t[:, t : t + 1] == wide_lane).astype(BF16)
        high[at, :] = jnp.broadcast_to(high_t[:, t : t + 1], (TILE, LANES))

    counts = count_ref[...].astype(F32)
    sums = dot(counts.astype(BF16), upper)
    before = jnp.zeros((1, 1), F32)
    rows = []
    for r in range(npass):
        rows.append(sums[r : r + 1, :] + before)
        before = before + sums[r : r + 1, LANES - 1 : LANES]
    ends = jnp.concatenate(rows, axis=0)
    starts[...] = (ends - counts).astype(I32)
    final = ends.astype(I32) - 1
    last = last_ref[...].astype(F32)
    fill_rows, end_rows = [], []
    for t in range(tiles + 1):
        hit = final == me * tiles + t
        fill_rows.append(jnp.sum(jnp.where(hit, last, 0.0), axis=0, keepdims=True))
        end_rows.append(jnp.sum(jnp.where(hit, 1.0, 0.0), axis=0, keepdims=True))
    fill = jnp.sum(jnp.concatenate(fill_rows, axis=0), axis=1, keepdims=True)
    ending = jnp.sum(jnp.concatenate(end_rows, axis=0), axis=1, keepdims=True)
    fills[...] = jnp.broadcast_to(jnp.where(ending > 0, fill, float(TILE))[:tiles], (tiles, LANES))
    goes = ending == 0
    join1[...] = jnp.broadcast_to(goes[:tiles].astype(F32), (tiles, LANES))
    join2[...] = jnp.broadcast_to(
        goes[:tiles].astype(F32) * goes[1 : tiles + 1].astype(F32), (tiles, LANES)
    )

    up = at_uv(lax.rem(u + 1, NY), v)
    down = at_uv(lax.rem(u + NY - 1, NY), v)
    across = index(x, y, other)
    n_up, n_down = NY - 1 - NY // 2, NY // 2

    def pass_on(block, where, send, recv):
        push(qb.at[block, c], qb.at[block, c], where, send, recv)

    arrived(qb.at[u, c, pl.ds(0, (NX - 1) * nq)], qx_recv)
    pass_on(u, up, qup_send, qup_recv.at[0])
    pass_on(u, down, qdn_send, qdn_recv.at[0])
    pass_on(u, across, qc_send, qc_recv)

    cent_copy.wait()
    half_lane = lax.broadcasted_iota(I32, (CAP, cent.shape[0]), 1).astype(F32)

    def ring(s):
        block = lax.rem(u + s, NY)
        arrived(qb.at[block, c], qdn_recv.at[s - 1])
        if s < n_down:
            pass_on(block, down, qdn_send, qdn_recv.at[s])
        pass_on(block, across, qc_send, qc_recv)
        if s <= n_up:
            block = lax.rem(u + NY - s, NY)
            arrived(qb.at[block, c], qup_recv.at[s - 1])
            if s < n_up:
                pass_on(block, up, qup_send, qup_recv.at[s])
            pass_on(block, across, qc_send, qc_recv)

    arrived(asked.at[pl.ds(0, NY * NC - 1)], ry_recv)
    for g in range(NY):
        wanted = jnp.concatenate(
            [asked[(a + g) % NY * NC + k, a : a + 1, :] for a, k in pairs], axis=0
        )
        wanted = wanted.astype(F32).T
        for j in range(group):
            onehot[pl.ds(j * CAP, CAP), :] = (wanted[:CAP, j : j + 1] == half_lane).astype(BF16)
        found = dot(onehot[...], cent[...]).astype(BF16)
        sent[pl.ds(g * gslots, gslots), :] = found
        if g == 0:
            fetched[pl.ds(0, CAP), :] = found[:CAP]
        for a, k in pairs:
            if (g, a, k) != (0, 0, 0):
                at = pl.ds((g * group + a * NC + k) * CAP, CAP)
                pltpu.make_async_remote_copy(
                    src_ref=sent.at[at],
                    dst_ref=fetched.at[at],
                    send_sem=row_send,
                    recv_sem=row_recv.at[g],
                    device_id={"psg": ahead(g, a, k)[2]},
                    device_id_type=MESH,
                ).start()
        if g % 2 == 0:
            ring(g // 2 + 1)

    code_copy.wait()

    @pl.loop(0, tiles)
    def _(t):
        at = pl.ds(pl.multiple_of(t * TILE, TILE), TILE)
        v = code[at, :]
        first = jnp.where(v == 0, bw_ref[0:1, :], bw_ref[1:2, :])
        second = jnp.where(v == 2, bw_ref[2:3, :], bw_ref[3:4, :])
        res[at, :] = jnp.where(v < 2, first, second)

    span = 4 * TILE
    for g in range(NY):
        count = (group - 1 if g == 0 else group) * CAP
        arrived(fetched.at[pl.ds(0, count)], row_recv.at[g])
        base = g * gslots
        both = jnp.concatenate(
            [fetched[pl.ds(base, 256), :], fetched[pl.ds(base + 256, 256), :]], axis=1
        )

        @pl.loop(0, tiles * TILE // span)
        def _(i):
            at = pl.ds(pl.multiple_of(i * span, span), span)
            picked = dot(low[at, :], both)
            which = high[at, :]
            keep = 0.0 if g == 0 else acc[at, :]
            keep = jnp.where(which == float(2 * g + 1), picked[:, LANES:], keep)
            acc[at, :] = jnp.where(which == float(2 * g), picked[:, :LANES], keep)

    @pl.loop(0, tiles)
    def _(t):
        at = pl.ds(pl.multiple_of(t * TILE, TILE), TILE)
        summed = acc[at, :] + res[at, :]
        scale = lax.rsqrt(jnp.sum(summed * summed, axis=1, keepdims=True) + EPS)
        unit = summed * scale
        unit = jnp.where(sub.astype(F32) < fills[pl.ds(t, 1), :], unit, unit[0:1, :])
        emb[at, :] = unit.astype(BF16)

    arrived(qb.at[pl.ds(0, NY), 0], qc_recv)

    span = tiles // 2
    chunk = 256
    per = qb.shape[2] // chunk

    def maxima(half):
        @pl.loop(0, NY * NC * per, unroll=8)
        def _(i):
            part = qb[
                i // (NC * per),
                lax.rem(i // per, NC),
                pl.ds(pl.multiple_of(lax.rem(i, per) * chunk, chunk), chunk),
                :,
            ]
            at = pl.ds(pl.multiple_of(i * chunk, chunk), chunk)
            s = dot(emb[pl.ds(half * span * TILE, span * TILE), :], part, 1, 1)
            top = jnp.max(s.reshape(span, TILE, chunk), axis=1)
            tm[pl.ds(half * span, span), at] = top
            if half == 0:
                head_out[:, at] = top[0:2, :]

    maxima(0)
    pltpu.make_async_remote_copy(
        src_ref=head_out,
        dst_ref=head_in,
        send_sem=head_send,
        recv_sem=head_recv,
        device_id={"psg": lax.rem(me + n - 1, n)},
        device_id_type=MESH,
    ).start()
    maxima(1)
    arrived(head_in, head_recv)
    tm[tiles : tiles + 2, :] = head_in[...]

    width = NX * LANES
    first_join, second_join = join1[...] > 0, join2[...] > 0
    for b in range(NY):
        stack = []
        for i in range(NX):
            at = pl.ds(b * width + i * LANES, LANES)
            one = tm[0:tiles, at]
            one = jnp.maximum(one, jnp.where(first_join, tm[1 : tiles + 1, at], one))
            one = jnp.maximum(one, jnp.where(second_join, tm[2 : tiles + 2, at], one))
            stack.append(one)
        turned = jnp.concatenate(stack, axis=0).T
        total = jnp.sum(turned.reshape(4, 32, LANES), axis=1)
        wide[b, 0] = total[0:2]
        wide[b, 1] = total[2:4]

    for d in range(1, NX):
        py, px = lax.rem(y + d, NY), lax.rem(x + d, NX)
        push(wide.at[py], mid.at[0, y], index(x, py, c), s1_send, s1_recv)
        push(wide.at[px], mid.at[1, x], index(px, y, c), s1_send, s1_recv)
    mid[0, y] = wide[y]
    mid[1, x] = wide[x]
    arrived(mid.at[:, pl.ds(0, NX - 1)], s1_recv)
    for j in range(1, NC * NX):
        k, d = j // NX, j % NX
        core = c if k == 0 else other
        px, py = lax.rem(x + d * (1 - core), NX), lax.rem(y + d * core, NY)
        parity = lax.rem(px + core * (py - px), 2)
        push(
            mid.at[core, :, parity],
            got.at[pl.ds(j * NY, NY)],
            index(px, py, core),
            s2_send,
            s2_recv,
        )
    got[0:NY] = mid[c, :, lax.rem(v, 2)]

    cand = cand_ref[...]
    tile = jnp.zeros(cand.shape, I32)
    for r in range(npass):
        table = jnp.broadcast_to(starts[r : r + 1, :], cand.shape)
        value = jnp.take_along_axis(table, cand & (LANES - 1), axis=1)
        tile = jnp.where(cand >> 7 == r, value, tile)
    owner, slot_of = tile // tiles, tile % tiles
    ox, oy = owner // (NY * NC), (owner // NC) % NY
    ou, ov = oy + c * (ox - oy), ox + c * (oy - ox)
    source = (((c - owner) & (NC - 1)) * NX + ((v - ov) & (NX - 1))) * NY + ou
    upper_half = lax.broadcasted_iota(I32, cand.shape, 0) < cand.shape[0] // 2
    turn = lax.rem(LANES - (c * (NX // 2) + v // 2) * tiles, LANES)

    arrived(got.at[pl.ds(0, n - NY)], s2_recv)
    tables = [pltpu.roll(got[:, i, :], turn, 1).T for i in range(2)]
    score = jnp.zeros(cand.shape, F32)
    for s in range(tiles):
        table = jnp.where(upper_half, tables[0][s : s + 1, :], tables[1][s : s + 1, :])
        value = jnp.take_along_axis(table, source, axis=1)
        score = jnp.where(slot_of == s, value, score)
    out_ref[...] = score

    arrived(req.at[pl.ds(0, NX - 1)], rx_send)
    arrived(asked.at[pl.ds(0, NY * NC - 1)], ry_send)
    arrived(sent.at[pl.ds(0, (n - 1) * CAP)], row_send)
    arrived(qb.at[0, 0, pl.ds(0, (NX - 1) * nq)], qx_send)
    arrived(qb.at[pl.ds(0, n_up), 0], qup_send)
    arrived(qb.at[pl.ds(0, n_down), 0], qdn_send)
    arrived(qb.at[pl.ds(0, NY), 0], qc_send)
    arrived(head_out, head_send)
    arrived(mid.at[:, pl.ds(0, NX - 1)], s1_send)
    arrived(got.at[pl.ds(0, n - NY)], s2_send)


def per_device(
    queries,
    candidates,
    centroids,
    bucket_weights,
    centroid_shard,
    centroid_row,
    residual_codes,
    tile_count,
    last_fill,
):
    n = NX * NY * NC
    tok, dim = residual_codes.shape
    tiles = tok // TILE
    nq = queries.shape[0] * queries.shape[1]
    ncand = candidates.size // LANES
    npass = tile_count.shape[0] // LANES
    dma = pltpu.SemaphoreType.DMA
    vmem = pl.BlockSpec(memory_space=pltpu.VMEM)
    anywhere = pl.BlockSpec(memory_space=pl.ANY)
    score = pl.pallas_call(
        kernel,
        out_shape=jax.ShapeDtypeStruct((ncand, LANES), F32),
        in_specs=[vmem, vmem, anywhere, anywhere, vmem, vmem, vmem, vmem, vmem],
        out_specs=vmem,
        scratch_shapes=[
            pltpu.VMEM(centroids.shape, BF16),
            pltpu.VMEM(residual_codes.shape, I32),
            pltpu.VMEM((NX, NY * NC, LANES), I32),
            pltpu.VMEM((NX, NY * NC, LANES), I32),
            pltpu.VMEM((NY * NC, NX, LANES), I32),
            pltpu.VMEM((NX * NC * CAP, centroids.shape[0]), BF16),
            pltpu.VMEM((n * CAP, dim), BF16),
            pltpu.VMEM((n * CAP, dim), BF16),
            pltpu.VMEM((tok, 256), BF16),
            pltpu.VMEM((tok, LANES), F32),
            pltpu.VMEM((tok, dim), F32),
            pltpu.VMEM((tok, dim), F32),
            pltpu.VMEM((tok, dim), BF16),
            pltpu.VMEM((NY, NC, NX * nq, dim), BF16),
            pltpu.VMEM((tiles + 8, n * nq), F32),
            pltpu.VMEM((2, n * nq), F32),
            pltpu.VMEM((2, n * nq), F32),
            pltpu.VMEM((NY, 2, 2, LANES), F32),
            pltpu.VMEM((NC, NY, 2, 2, LANES), F32),
            pltpu.VMEM((n, 2, LANES), F32),
            pltpu.VMEM((npass, LANES), I32),
            pltpu.VMEM((tiles, LANES), F32),
            pltpu.VMEM((tiles, LANES), F32),
            pltpu.VMEM((tiles, LANES), F32),
            dma((2,)),
            *[dma] * 5,
            dma((NY,)),
            dma,
            dma,
            dma,
            dma((NY // 2,)),
            dma,
            dma((NY // 2,)),
            *[dma] * 8,
        ],
        compiler_params=pltpu.CompilerParams(collective_id=0, has_side_effects=True),
    )(
        centroid_shard.reshape(tiles, TILE),
        centroid_row.reshape(tiles, TILE),
        centroids,
        residual_codes,
        bucket_weights,
        tile_count.reshape(npass, LANES),
        last_fill.reshape(npass, LANES),
        queries.reshape(nq, dim),
        candidates.reshape(ncand, LANES),
    )
    return score.reshape(candidates.shape)


def solution(mesh):
    both = ("groups", "psg")
    return jax.shard_map(
        per_device,
        mesh=mesh,
        in_specs=(
            P(both, None, None),
            P(both, None),
            P("psg", None),
            P(),
            P("psg", None),
            P("psg"),
            P("psg", None),
            P(),
            P(),
        ),
        out_specs=P(both, None),
        check_vma=False,
    )
```

```python
import functools

import jax
import jax.numpy as jnp
from jax import lax
from jax.experimental import pallas as pl
from jax.experimental.pallas import tpu as pltpu
from jax.sharding import PartitionSpec as P

MESH = pl.DeviceIdType.MESH
TILE = 128
LANES = 128
NX, NY, NC = 8, 8, 2
CAP = 32
EPS = 1e-06
F32, BF16, I32 = jnp.float32, jnp.bfloat16, jnp.int32


def dot(a, b, ca=1, cb=0):
    return lax.dot_general(a, b, (((ca,), (cb,)), ((), ())), preferred_element_type=F32)


def kernel(
    owner_ref,
    row_ref,
    cent_hbm,
    code_hbm,
    bw_ref,
    count_ref,
    last_ref,
    query_ref,
    cand_ref,
    out_ref,
    cent,
    code,
    req,
    mid_req,
    asked,
    onehot,
    sent,
    fetched,
    low,
    high,
    res,
    acc,
    emb,
    qb,
    tm,
    head_out,
    head_in,
    wide,
    got,
    starts,
    fills,
    join1,
    join2,
    load_sem,
    rx_send,
    rx_recv,
    ry_send,
    ry_recv,
    row_send,
    row_recv,
    qx_send,
    qx_recv,
    qup_send,
    qup_recv,
    qdn_send,
    qdn_recv,
    qc_send,
    qc_recv,
    head_send,
    head_recv,
    score_send,
    score_recv,
):
    n = NX * NY * NC
    tiles = owner_ref.shape[0]
    npass = count_ref.shape[0]
    me = lax.axis_index("psg")
    x = me // (NY * NC)
    y = lax.rem(me // NC, NY)
    c = lax.rem(me, NC)
    other = 1 - c

    def index(px, py, pc):
        return (px * NY + py) * NC + pc

    def ahead(g, a, k):
        px, py = lax.rem(x + a, NX), lax.rem(y + a + g, NY)
        return px, py, index(px, py, c if k == 0 else other)

    def shift(device):
        dx = (x - device // (NY * NC)) & (NX - 1)
        dy = (y - (device // NC) % NY) & (NY - 1)
        dc = (c - device) & (NC - 1)
        return dx, dy, dc

    def push(src, dst, where, send, recv):
        pltpu.make_async_remote_copy(
            src_ref=src,
            dst_ref=dst,
            send_sem=send,
            recv_sem=recv,
            device_id={"psg": where},
            device_id_type=MESH,
        ).start()

    def arrived(ref, sem):
        pltpu.make_async_copy(ref, ref, sem).wait()

    def at_uv(u, v):
        return (1 - c) * index(v, u, 0) + c * index(u, v, 1)

    u, v = y + c * (x - y), x + c * (y - x)

    pairs = [(a, k) for a in range(NX) for k in range(NC)]
    far = sorted(
        [(g, a, k) for g in range(NY) for a, k in pairs if (g, a, k) != (0, 0, 0)],
        key=lambda p: -min(p[1], NX - p[1]) - min((p[0] + p[1]) % NY, -(p[0] + p[1]) % NY),
    )
    group = NX * NC
    gslots = group * CAP

    barrier = pltpu.get_barrier_semaphore()
    for g in range(NY):
        for a, k in pairs:
            if (g, a, k) != (0, 0, 0):
                pl.semaphore_signal(
                    barrier, inc=1, device_id={"psg": ahead(g, a, k)[2]}, device_id_type=MESH
                )
    cent_copy = pltpu.make_async_copy(cent_hbm, cent, load_sem.at[0])
    cent_copy.start()
    code_copy = pltpu.make_async_copy(code_hbm, code, load_sem.at[1])
    code_copy.start()

    sub = lax.broadcasted_iota(I32, (LANES, LANES), 0)
    lane = lax.broadcasted_iota(I32, (LANES, LANES), 1)
    upper = (sub <= lane).astype(BF16)
    ones = jnp.ones((LANES, LANES), BF16)
    dx, dy, dc = shift(owner_ref[...])
    rel = (dx * NY + dy) * NC + dc
    turn_of = ((dy - dx) & (NY - 1)) * (NX * NC) + dx * NC + dc
    crow = row_ref[...]
    carry = jnp.zeros((LANES, LANES), F32)
    low_sum = jnp.zeros((LANES, LANES), F32)
    high_sum = jnp.zeros((LANES, LANES), F32)
    slots = []
    for t in range(tiles):
        member = sub == rel[t : t + 1, :]
        flags = member.astype(BF16)
        running = dot(flags, upper) + carry
        carry = carry + dot(flags, ones)
        rank = jnp.sum(jnp.where(member, running, 0.0), axis=0, keepdims=True).astype(I32) - 1
        slots.append(turn_of[t : t + 1, :] * CAP + rank)
        place = sub == rank
        tok = crow[t : t + 1, :]
        low_sum = low_sum + dot(
            flags, jnp.where(place, (tok & 255).astype(F32), 0.0).astype(BF16), 1, 1
        )
        high_sum = high_sum + dot(
            flags, jnp.where(place, (tok >> 8).astype(F32), 0.0).astype(BF16), 1, 1
        )
    asking = (low_sum + 256.0 * high_sum).astype(I32)
    req[...] = asking.reshape(NX, NY * NC, LANES)

    pl.semaphore_wait(barrier, n - 1)

    for a in range(1, NX):
        where = index(lax.rem(x + NX - a, NX), y, c)
        push(req.at[a], mid_req.at[a], where, rx_send, rx_recv)
    mid_req[0] = req[0]

    nq = query_ref.shape[0]
    own_block = qb.at[u, c, pl.ds(pl.multiple_of(v * nq, nq), nq)]
    for a in range(1, NX):
        push(query_ref, own_block, at_uv(u, lax.rem(v + a, NX)), qx_send, qx_recv)
    qb[u, c, pl.ds(pl.multiple_of(v * nq, nq), nq), :] = query_ref[...]

    arrived(mid_req.at[pl.ds(0, NX - 1)], rx_recv)
    for j in range(1, NY * NC):
        d, k = j // NC, j % NC
        where = index(x, lax.rem(y + NY - d, NY), c if k == 0 else other)
        push(mid_req.at[:, j], asked.at[j], where, ry_send, ry_recv)
    asked[0] = mid_req[:, 0, :]

    up = at_uv(lax.rem(u + 1, NY), v)
    down = at_uv(lax.rem(u + NY - 1, NY), v)
    across = index(x, y, other)
    n_up, n_down = NY - 1 - NY // 2, NY // 2

    def pass_on(block, where, send, recv):
        push(qb.at[block, c], qb.at[block, c], where, send, recv)

    arrived(qb.at[u, c, pl.ds(0, (NX - 1) * nq)], qx_recv)
    pass_on(u, up, qup_send, qup_recv.at[0])
    pass_on(u, down, qdn_send, qdn_recv.at[0])
    pass_on(u, across, qc_send, qc_recv)

    cent_copy.wait()
    half_lane = lax.broadcasted_iota(I32, (CAP, cent.shape[0]), 1).astype(F32)

    def ring(s):
        block = lax.rem(u + s, NY)
        arrived(qb.at[block, c], qdn_recv.at[s - 1])
        if s < n_down:
            pass_on(block, down, qdn_send, qdn_recv.at[s])
        pass_on(block, across, qc_send, qc_recv)
        if s <= n_up:
            block = lax.rem(u + NY - s, NY)
            arrived(qb.at[block, c], qup_recv.at[s - 1])
            if s < n_up:
                pass_on(block, up, qup_send, qup_recv.at[s])
            pass_on(block, across, qc_send, qc_recv)

    ring(1)
    arrived(asked.at[pl.ds(0, NY * NC - 1)], ry_recv)
    for g in range(NY):
        wanted = jnp.concatenate(
            [asked[(a + g) % NY * NC + k, a : a + 1, :] for a, k in pairs], axis=0
        )
        wanted = wanted.astype(F32).T
        for j in range(group):
            onehot[pl.ds(j * CAP, CAP), :] = (wanted[:CAP, j : j + 1] == half_lane).astype(BF16)
        found = dot(onehot[...], cent[...]).astype(BF16)
        sent[pl.ds(g * gslots, gslots), :] = found
        if g == 0:
            fetched[pl.ds(0, CAP), :] = found[:CAP]
        for a, k in pairs:
            if (g, a, k) != (0, 0, 0):
                at = pl.ds((g * group + a * NC + k) * CAP, CAP)
                pltpu.make_async_remote_copy(
                    src_ref=sent.at[at],
                    dst_ref=fetched.at[at],
                    send_sem=row_send,
                    recv_sem=row_recv.at[g],
                    device_id={"psg": ahead(g, a, k)[2]},
                    device_id_type=MESH,
                ).start()
        if g == 3:
            ring(2)

    ring(3)
    slot = jnp.concatenate(slots, axis=0)
    pad = jnp.zeros((LANES - tiles, LANES), F32)
    low_t = jnp.concatenate([(slot & 255).astype(F32), pad], axis=0).T
    high_t = jnp.concatenate([(slot >> 8).astype(F32), pad], axis=0).T
    wide_lane = lax.broadcasted_iota(I32, (LANES, 256), 1).astype(F32)
    for t in range(tiles):
        at = pl.ds(t * TILE, TILE)
        low[at, :] = (low_t[:, t : t + 1] == wide_lane).astype(BF16)
        high[at, :] = jnp.broadcast_to(high_t[:, t : t + 1], (TILE, LANES))

    counts = count_ref[...].astype(F32)
    sums = dot(counts.astype(BF16), upper)
    before = jnp.zeros((1, 1), F32)
    rows = []
    for r in range(npass):
        rows.append(sums[r : r + 1, :] + before)
        before = before + sums[r : r + 1, LANES - 1 : LANES]
    ends = jnp.concatenate(rows, axis=0)
    starts[...] = (ends - counts).astype(I32)
    final = ends.astype(I32) - 1
    last = last_ref[...].astype(F32)
    fill_rows, end_rows = [], []
    for t in range(tiles + 1):
        hit = final == me * tiles + t
        fill_rows.append(jnp.sum(jnp.where(hit, last, 0.0), axis=0, keepdims=True))
        end_rows.append(jnp.sum(jnp.where(hit, 1.0, 0.0), axis=0, keepdims=True))
    fill = jnp.sum(jnp.concatenate(fill_rows, axis=0), axis=1, keepdims=True)
    ending = jnp.sum(jnp.concatenate(end_rows, axis=0), axis=1, keepdims=True)
    fills[...] = jnp.broadcast_to(jnp.where(ending > 0, fill, float(TILE))[:tiles], (tiles, LANES))
    goes = ending == 0
    join1[...] = jnp.broadcast_to(goes[:tiles].astype(F32), (tiles, LANES))
    join2[...] = jnp.broadcast_to(
        goes[:tiles].astype(F32) * goes[1 : tiles + 1].astype(F32), (tiles, LANES)
    )

    code_copy.wait()

    @pl.loop(0, tiles, unroll=4)
    def _(t):
        at = pl.ds(pl.multiple_of(t * TILE, TILE), TILE)
        v = code[at, :]
        first = jnp.where(v == 0, bw_ref[0:1, :], bw_ref[1:2, :])
        second = jnp.where(v == 2, bw_ref[2:3, :], bw_ref[3:4, :])
        res[at, :] = jnp.where(v < 2, first, second)

    cand = cand_ref[...]
    tile = jnp.zeros(cand.shape, I32)
    for r in range(npass):
        table = jnp.broadcast_to(starts[r : r + 1, :], cand.shape)
        value = jnp.take_along_axis(table, cand & (LANES - 1), axis=1)
        tile = jnp.where(cand >> 7 == r, value, tile)
    ring(4)

    span = 4 * TILE
    for g in range(NY):
        count = (group - 1 if g == 0 else group) * CAP
        arrived(fetched.at[pl.ds(0, count)], row_recv.at[g])
        base = g * gslots
        both = jnp.concatenate(
            [fetched[pl.ds(base, 256), :], fetched[pl.ds(base + 256, 256), :]], axis=1
        )

        @pl.loop(0, tiles * TILE // span, unroll=4)
        def _(i):
            at = pl.ds(pl.multiple_of(i * span, span), span)
            picked = dot(low[at, :], both)
            which = high[at, :]
            keep = 0.0 if g == 0 else acc[at, :]
            keep = jnp.where(which == float(2 * g + 1), picked[:, LANES:], keep)
            acc[at, :] = jnp.where(which == float(2 * g), picked[:, :LANES], keep)

    @pl.loop(0, tiles, unroll=8)
    def _(t):
        at = pl.ds(pl.multiple_of(t * TILE, TILE), TILE)
        summed = acc[at, :] + res[at, :]
        scale = lax.rsqrt(jnp.sum(summed * summed, axis=1, keepdims=True) + EPS)
        unit = summed * scale
        unit = jnp.where(sub.astype(F32) < fills[pl.ds(t, 1), :], unit, unit[0:1, :])
        emb[at, :] = unit.astype(BF16)

    arrived(qb.at[pl.ds(0, NY), 0], qc_recv)

    span = tiles // 2
    chunk = 256
    per = qb.shape[2] // chunk

    def maxima(half):
        @pl.loop(0, NY * NC * per, unroll=8)
        def _(i):
            part = qb[
                i // (NC * per),
                lax.rem(i // per, NC),
                pl.ds(pl.multiple_of(lax.rem(i, per) * chunk, chunk), chunk),
                :,
            ]
            at = pl.ds(pl.multiple_of(i * chunk, chunk), chunk)
            s = dot(emb[pl.ds(half * span * TILE, span * TILE), :], part, 1, 1)
            top = jnp.max(s.reshape(span, TILE, chunk), axis=1)
            tm[pl.ds(half * span, span), at] = top
            if half == 0:
                head_out[:, at] = top[0:2, :]

    maxima(0)
    pltpu.make_async_remote_copy(
        src_ref=head_out,
        dst_ref=head_in,
        send_sem=head_send,
        recv_sem=head_recv,
        device_id={"psg": lax.rem(me + n - 1, n)},
        device_id_type=MESH,
    ).start()
    maxima(1)
    arrived(head_in, head_recv)
    tm[tiles : tiles + 2, :] = head_in[...]

    width = NX * LANES
    first_join, second_join = join1[...] > 0, join2[...] > 0
    for b in range(NY):
        stack = []
        for i in range(NX):
            at = pl.ds(b * width + i * LANES, LANES)
            one = tm[0:tiles, at]
            one = jnp.maximum(one, jnp.where(first_join, tm[1 : tiles + 1, at], one))
            one = jnp.maximum(one, jnp.where(second_join, tm[2 : tiles + 2, at], one))
            stack.append(one)
        turned = jnp.concatenate(stack, axis=0).T
        total = jnp.sum(turned.reshape(4, 32, LANES), axis=1)
        wide[b, 0] = total[0:2]
        wide[b, 1] = total[2:4]

    for g, a, k in far:
        px, py, peer = ahead(g, a, k)
        pc = c if k == 0 else other
        pu, pv = py + pc * (px - py), px + pc * (py - px)
        push(
            wide.at[pu, lax.rem(pv, 2)],
            got.at[g * group + a * NC + k],
            peer,
            score_send,
            score_recv,
        )
    got[0] = wide[u, lax.rem(v, 2)]

    owner, slot_of = tile // tiles, tile % tiles
    dx, dy, dc = shift(owner)
    source = ((dy - dx) & (NY - 1)) * (NX * NC) + dx * NC + dc
    upper_half = lax.broadcasted_iota(I32, cand.shape, 0) < cand.shape[0] // 2
    turn = lax.rem(LANES - (c * (NX // 2) + v // 2) * tiles, LANES)

    arrived(got.at[pl.ds(0, n - 1)], score_recv)
    tables = [pltpu.roll(got[:, i, :], turn, 1).T for i in range(2)]
    score = jnp.zeros(cand.shape, F32)
    for s in range(tiles):
        table = jnp.where(upper_half, tables[0][s : s + 1, :], tables[1][s : s + 1, :])
        value = jnp.take_along_axis(table, source, axis=1)
        score = jnp.where(slot_of == s, value, score)
    out_ref[...] = score

    arrived(req.at[pl.ds(0, NX - 1)], rx_send)
    arrived(asked.at[pl.ds(0, NY * NC - 1)], ry_send)
    arrived(sent.at[pl.ds(0, (n - 1) * CAP)], row_send)
    arrived(qb.at[0, 0, pl.ds(0, (NX - 1) * nq)], qx_send)
    arrived(qb.at[pl.ds(0, n_up), 0], qup_send)
    arrived(qb.at[pl.ds(0, n_down), 0], qdn_send)
    arrived(qb.at[pl.ds(0, NY), 0], qc_send)
    arrived(head_out, head_send)
    arrived(got.at[pl.ds(0, n - 1)], score_send)


def per_device(
    queries,
    candidates,
    centroids,
    bucket_weights,
    centroid_shard,
    centroid_row,
    residual_codes,
    tile_count,
    last_fill,
):
    n = NX * NY * NC
    tok, dim = residual_codes.shape
    tiles = tok // TILE
    nq = queries.shape[0] * queries.shape[1]
    ncand = candidates.size // LANES
    npass = tile_count.shape[0] // LANES
    dma = pltpu.SemaphoreType.DMA
    vmem = pl.BlockSpec(memory_space=pltpu.VMEM)
    anywhere = pl.BlockSpec(memory_space=pl.ANY)
    score = pl.pallas_call(
        kernel,
        out_shape=jax.ShapeDtypeStruct((ncand, LANES), F32),
        in_specs=[vmem, vmem, anywhere, anywhere, vmem, vmem, vmem, vmem, vmem],
        out_specs=vmem,
        scratch_shapes=[
            pltpu.VMEM(centroids.shape, BF16),
            pltpu.VMEM(residual_codes.shape, I32),
            pltpu.VMEM((NX, NY * NC, LANES), I32),
            pltpu.VMEM((NX, NY * NC, LANES), I32),
            pltpu.VMEM((NY * NC, NX, LANES), I32),
            pltpu.VMEM((NX * NC * CAP, centroids.shape[0]), BF16),
            pltpu.VMEM((n * CAP, dim), BF16),
            pltpu.VMEM((n * CAP, dim), BF16),
            pltpu.VMEM((tok, 256), BF16),
            pltpu.VMEM((tok, LANES), F32),
            pltpu.VMEM((tok, dim), F32),
            pltpu.VMEM((tok, dim), F32),
            pltpu.VMEM((tok, dim), BF16),
            pltpu.VMEM((NY, NC, NX * nq, dim), BF16),
            pltpu.VMEM((tiles + 8, n * nq), F32),
            pltpu.VMEM((2, n * nq), F32),
            pltpu.VMEM((2, n * nq), F32),
            pltpu.VMEM((NY, 2, 2, LANES), F32),
            pltpu.VMEM((n, 2, LANES), F32),
            pltpu.VMEM((npass, LANES), I32),
            pltpu.VMEM((tiles, LANES), F32),
            pltpu.VMEM((tiles, LANES), F32),
            pltpu.VMEM((tiles, LANES), F32),
            dma((2,)),
            *[dma] * 5,
            dma((NY,)),
            dma,
            dma,
            dma,
            dma((NY // 2,)),
            dma,
            dma((NY // 2,)),
            *[dma] * 6,
        ],
        compiler_params=pltpu.CompilerParams(collective_id=0, has_side_effects=True),
    )(
        centroid_shard.reshape(tiles, TILE),
        centroid_row.reshape(tiles, TILE),
        centroids,
        residual_codes,
        bucket_weights,
        tile_count.reshape(npass, LANES),
        last_fill.reshape(npass, LANES),
        queries.reshape(nq, dim),
        candidates.reshape(ncand, LANES),
    )
    return score.reshape(candidates.shape)


def solution(mesh):
    both = ("groups", "psg")
    return jax.shard_map(
        per_device,
        mesh=mesh,
        in_specs=(
            P(both, None, None),
            P(both, None),
            P("psg", None),
            P(),
            P("psg", None),
            P("psg"),
            P("psg", None),
            P(),
            P(),
        ),
        out_specs=P(both, None),
        check_vma=False,
    )
```

```python
import functools

import jax
import jax.numpy as jnp
from jax import lax
from jax.experimental import pallas as pl
from jax.experimental.pallas import tpu as pltpu
from jax.sharding import PartitionSpec as P

MESH = pl.DeviceIdType.MESH
TILE = 128
LANES = 128
NX, NY, NC = 8, 8, 2
CAP = 32
EPS = 1e-06
F32, BF16, I32 = jnp.float32, jnp.bfloat16, jnp.int32


def dot(a, b, ca=1, cb=0):
    return lax.dot_general(a, b, (((ca,), (cb,)), ((), ())), preferred_element_type=F32)


def kernel(
    owner_ref,
    row_ref,
    cent_hbm,
    code_hbm,
    bw_ref,
    count_ref,
    last_ref,
    query_ref,
    cand_ref,
    out_ref,
    cent,
    code,
    req,
    mid_req,
    asked,
    onehot,
    sent,
    fetched,
    low,
    high,
    res,
    acc,
    emb,
    qb,
    tm,
    head_out,
    head_in,
    wide,
    got,
    starts,
    fills,
    join1,
    join2,
    load_sem,
    rx_send,
    rx_recv,
    ry_send,
    ry_recv,
    row_send,
    row_recv,
    qx_send,
    qx_recv,
    qup_send,
    qup_recv,
    qdn_send,
    qdn_recv,
    qc_send,
    qc_recv,
    head_send,
    head_recv,
    score_send,
    score_recv,
):
    n = NX * NY * NC
    tiles = owner_ref.shape[0]
    npass = count_ref.shape[0]
    me = lax.axis_index("psg")
    x = me // (NY * NC)
    y = lax.rem(me // NC, NY)
    c = lax.rem(me, NC)
    other = 1 - c

    def index(px, py, pc):
        return (px * NY + py) * NC + pc

    def ahead(g, a, k):
        px, py = lax.rem(x + a, NX), lax.rem(y + a + g, NY)
        return px, py, index(px, py, c if k == 0 else other)

    def shift(device):
        dx = (x - device // (NY * NC)) & (NX - 1)
        dy = (y - (device // NC) % NY) & (NY - 1)
        dc = (c - device) & (NC - 1)
        return dx, dy, dc

    def push(src, dst, where, send, recv):
        pltpu.make_async_remote_copy(
            src_ref=src,
            dst_ref=dst,
            send_sem=send,
            recv_sem=recv,
            device_id={"psg": where},
            device_id_type=MESH,
        ).start()

    def arrived(ref, sem):
        pltpu.make_async_copy(ref, ref, sem).wait()

    def at_uv(u, v):
        return (1 - c) * index(v, u, 0) + c * index(u, v, 1)

    u, v = y + c * (x - y), x + c * (y - x)

    pairs = [(a, k) for a in range(NX) for k in range(NC)]
    far = sorted(
        [(g, a, k) for g in range(NY) for a, k in pairs if (g, a, k) != (0, 0, 0)],
        key=lambda p: -min(p[1], NX - p[1]) - min((p[0] + p[1]) % NY, -(p[0] + p[1]) % NY),
    )
    group = NX * NC
    gslots = group * CAP

    barrier = pltpu.get_barrier_semaphore()
    greeted = [index(lax.rem(x + d, NX), y, c) for d in range(1, NX)]
    greeted += [
        index(x, lax.rem(y + d, NY), c if k == 0 else other)
        for d in range(NY)
        for k in range(NC)
        if (d, k) != (0, 0)
    ]
    for peer in greeted:
        pl.semaphore_signal(barrier, inc=1, device_id={"psg": peer}, device_id_type=MESH)
    cent_copy = pltpu.make_async_copy(cent_hbm, cent, load_sem.at[0])
    cent_copy.start()
    code_copy = pltpu.make_async_copy(code_hbm, code, load_sem.at[1])
    code_copy.start()

    sub = lax.broadcasted_iota(I32, (LANES, LANES), 0)
    lane = lax.broadcasted_iota(I32, (LANES, LANES), 1)
    upper = (sub <= lane).astype(BF16)
    ones = jnp.ones((LANES, LANES), BF16)
    dx, dy, dc = shift(owner_ref[...])
    rel = (dx * NY + dy) * NC + dc
    turn_of = ((dy - dx) & (NY - 1)) * (NX * NC) + dx * NC + dc
    crow = row_ref[...]
    members = [sub == rel[t : t + 1, :] for t in range(tiles)]
    flags = [m.astype(BF16) for m in members]
    running = dot(jnp.concatenate(flags, axis=0), jnp.concatenate([upper, ones], axis=1))
    carry = jnp.zeros((LANES, LANES), F32)
    slots, lows, highs = [], [], []
    for t in range(tiles):
        part = running[t * LANES : (t + 1) * LANES, :]
        count = jnp.where(members[t], part[:, :LANES] + carry, 0.0)
        carry = carry + part[:, LANES:]
        rank = jnp.sum(count, axis=0, keepdims=True).astype(I32) - 1
        slots.append(turn_of[t : t + 1, :] * CAP + rank)
        place = sub == rank
        tok = crow[t : t + 1, :]
        lows.append(jnp.where(place, (tok & 255).astype(F32), 0.0).astype(BF16))
        highs.append(jnp.where(place, (tok >> 8).astype(F32), 0.0).astype(BF16))
    values = jnp.concatenate(
        [jnp.concatenate(lows, axis=1), jnp.concatenate(highs, axis=1)], axis=0
    )
    summed = dot(jnp.concatenate(flags, axis=1), values, 1, 1)
    low_sum, high_sum = summed[:, :LANES], summed[:, LANES:]
    asking = (low_sum + 256.0 * high_sum).astype(I32)
    req[...] = asking.reshape(NX, NY * NC, LANES)

    pl.semaphore_wait(barrier, len(greeted))

    for a in range(1, NX):
        where = index(lax.rem(x + NX - a, NX), y, c)
        push(req.at[a], mid_req.at[a], where, rx_send, rx_recv)
    mid_req[0] = req[0]

    nq = query_ref.shape[0]
    own_block = qb.at[u, c, pl.ds(pl.multiple_of(v * nq, nq), nq)]
    for a in range(1, NX):
        push(query_ref, own_block, at_uv(u, lax.rem(v + a, NX)), qx_send, qx_recv)
    qb[u, c, pl.ds(pl.multiple_of(v * nq, nq), nq), :] = query_ref[...]

    arrived(mid_req.at[pl.ds(0, NX - 1)], rx_recv)
    for j in range(1, NY * NC):
        d, k = j // NC, j % NC
        where = index(x, lax.rem(y + NY - d, NY), c if k == 0 else other)
        push(mid_req.at[:, j], asked.at[j], where, ry_send, ry_recv)
    asked[0] = mid_req[:, 0, :]

    up = at_uv(lax.rem(u + 1, NY), v)
    down = at_uv(lax.rem(u + NY - 1, NY), v)
    across = index(x, y, other)
    n_up, n_down = NY - 1 - NY // 2, NY // 2

    def pass_on(block, where, send, recv):
        push(qb.at[block, c], qb.at[block, c], where, send, recv)

    arrived(qb.at[u, c, pl.ds(0, (NX - 1) * nq)], qx_recv)
    pass_on(u, up, qup_send, qup_recv.at[0])
    pass_on(u, down, qdn_send, qdn_recv.at[0])
    pass_on(u, across, qc_send, qc_recv)

    cent_copy.wait()
    half_lane = lax.broadcasted_iota(I32, (CAP, cent.shape[0]), 1).astype(F32)

    def ring(s):
        block = lax.rem(u + s, NY)
        arrived(qb.at[block, c], qdn_recv.at[s - 1])
        if s < n_down:
            pass_on(block, down, qdn_send, qdn_recv.at[s])
        pass_on(block, across, qc_send, qc_recv)
        if s <= n_up:
            block = lax.rem(u + NY - s, NY)
            arrived(qb.at[block, c], qup_recv.at[s - 1])
            if s < n_up:
                pass_on(block, up, qup_send, qup_recv.at[s])
            pass_on(block, across, qc_send, qc_recv)

    ring(1)
    arrived(asked.at[pl.ds(0, NY * NC - 1)], ry_recv)
    for g in range(NY):
        wanted = jnp.concatenate(
            [asked[(a + g) % NY * NC + k, a : a + 1, :] for a, k in pairs], axis=0
        )
        wanted = wanted.astype(F32).T
        for j in range(group):
            onehot[pl.ds(j * CAP, CAP), :] = (wanted[:CAP, j : j + 1] == half_lane).astype(BF16)
        found = dot(onehot[...], cent[...]).astype(BF16)
        sent[pl.ds(g * gslots, gslots), :] = found
        if g == 0:
            fetched[pl.ds(0, CAP), :] = found[:CAP]
        for a, k in pairs:
            if (g, a, k) != (0, 0, 0):
                at = pl.ds((g * group + a * NC + k) * CAP, CAP)
                pltpu.make_async_remote_copy(
                    src_ref=sent.at[at],
                    dst_ref=fetched.at[at],
                    send_sem=row_send,
                    recv_sem=row_recv.at[g],
                    device_id={"psg": ahead(g, a, k)[2]},
                    device_id_type=MESH,
                ).start()
        if g == 3:
            ring(2)

    ring(3)
    slot = jnp.concatenate(slots, axis=0)
    pad = jnp.zeros((LANES - tiles, LANES), F32)
    low_t = jnp.concatenate([(slot & 255).astype(F32), pad], axis=0).T
    high_t = jnp.concatenate([(slot >> 8).astype(F32), pad], axis=0).T
    wide_lane = lax.broadcasted_iota(I32, (LANES, 256), 1).astype(F32)
    for t in range(tiles):
        at = pl.ds(t * TILE, TILE)
        low[at, :] = (low_t[:, t : t + 1] == wide_lane).astype(BF16)
        high[at, :] = jnp.broadcast_to(high_t[:, t : t + 1], (TILE, LANES))

    counts = count_ref[...].astype(F32)
    sums = dot(counts.astype(BF16), upper)
    before = jnp.zeros((1, 1), F32)
    rows = []
    for r in range(npass):
        rows.append(sums[r : r + 1, :] + before)
        before = before + sums[r : r + 1, LANES - 1 : LANES]
    ends = jnp.concatenate(rows, axis=0)
    starts[...] = (ends - counts).astype(I32)
    final = ends.astype(I32) - 1
    last = last_ref[...].astype(F32)
    fill_rows, end_rows = [], []
    for t in range(tiles + 1):
        hit = final == me * tiles + t
        fill_rows.append(jnp.sum(jnp.where(hit, last, 0.0), axis=0, keepdims=True))
        end_rows.append(jnp.sum(jnp.where(hit, 1.0, 0.0), axis=0, keepdims=True))
    fill = jnp.sum(jnp.concatenate(fill_rows, axis=0), axis=1, keepdims=True)
    ending = jnp.sum(jnp.concatenate(end_rows, axis=0), axis=1, keepdims=True)
    fills[...] = jnp.broadcast_to(jnp.where(ending > 0, fill, float(TILE))[:tiles], (tiles, LANES))
    goes = ending == 0
    join1[...] = jnp.broadcast_to(goes[:tiles].astype(F32), (tiles, LANES))
    join2[...] = jnp.broadcast_to(
        goes[:tiles].astype(F32) * goes[1 : tiles + 1].astype(F32), (tiles, LANES)
    )

    code_copy.wait()

    @pl.loop(0, tiles, unroll=4)
    def _(t):
        at = pl.ds(pl.multiple_of(t * TILE, TILE), TILE)
        v = code[at, :]
        first = jnp.where(v == 0, bw_ref[0:1, :], bw_ref[1:2, :])
        second = jnp.where(v == 2, bw_ref[2:3, :], bw_ref[3:4, :])
        res[at, :] = jnp.where(v < 2, first, second)

    cand = cand_ref[...]
    tile = jnp.zeros(cand.shape, I32)
    for r in range(npass):
        table = jnp.broadcast_to(starts[r : r + 1, :], cand.shape)
        value = jnp.take_along_axis(table, cand & (LANES - 1), axis=1)
        tile = jnp.where(cand >> 7 == r, value, tile)
    ring(4)

    span = 4 * TILE
    for g in range(NY):
        count = (group - 1 if g == 0 else group) * CAP
        arrived(fetched.at[pl.ds(0, count)], row_recv.at[g])
        base = g * gslots
        both = jnp.concatenate(
            [fetched[pl.ds(base, 256), :], fetched[pl.ds(base + 256, 256), :]], axis=1
        )

        @pl.loop(0, tiles * TILE // span, unroll=4)
        def _(i):
            at = pl.ds(pl.multiple_of(i * span, span), span)
            picked = dot(low[at, :], both)
            which = high[at, :]
            keep = 0.0 if g == 0 else acc[at, :]
            keep = jnp.where(which == float(2 * g + 1), picked[:, LANES:], keep)
            acc[at, :] = jnp.where(which == float(2 * g), picked[:, :LANES], keep)

    @pl.loop(0, tiles, unroll=8)
    def _(t):
        at = pl.ds(pl.multiple_of(t * TILE, TILE), TILE)
        summed = acc[at, :] + res[at, :]
        scale = lax.rsqrt(jnp.sum(summed * summed, axis=1, keepdims=True) + EPS)
        unit = summed * scale
        unit = jnp.where(sub.astype(F32) < fills[pl.ds(t, 1), :], unit, unit[0:1, :])
        emb[at, :] = unit.astype(BF16)

    arrived(qb.at[pl.ds(0, NY), 0], qc_recv)

    span = tiles // 2
    chunk = 256
    per = qb.shape[2] // chunk

    def maxima(half):
        @pl.loop(0, NY * NC * per, unroll=16)
        def _(i):
            part = qb[
                i // (NC * per),
                lax.rem(i // per, NC),
                pl.ds(pl.multiple_of(lax.rem(i, per) * chunk, chunk), chunk),
                :,
            ]
            at = pl.ds(pl.multiple_of(i * chunk, chunk), chunk)
            s = dot(emb[pl.ds(half * span * TILE, span * TILE), :], part, 1, 1)
            top = jnp.max(s.reshape(span, TILE, chunk), axis=1)
            tm[pl.ds(half * span, span), at] = top
            if half == 0:
                head_out[:, at] = top[0:2, :]

    maxima(0)
    pltpu.make_async_remote_copy(
        src_ref=head_out,
        dst_ref=head_in,
        send_sem=head_send,
        recv_sem=head_recv,
        device_id={"psg": lax.rem(me + n - 1, n)},
        device_id_type=MESH,
    ).start()
    maxima(1)
    arrived(head_in, head_recv)
    tm[tiles : tiles + 2, :] = head_in[...]

    width = NX * LANES
    first_join, second_join = join1[...] > 0, join2[...] > 0
    for b in range(NY):
        stack = []
        for i in range(NX):
            at = pl.ds(b * width + i * LANES, LANES)
            one = tm[0:tiles, at]
            one = jnp.maximum(one, jnp.where(first_join, tm[1 : tiles + 1, at], one))
            one = jnp.maximum(one, jnp.where(second_join, tm[2 : tiles + 2, at], one))
            stack.append(one)
        turned = jnp.concatenate(stack, axis=0).T
        total = jnp.sum(turned.reshape(4, 32, LANES), axis=1)
        wide[b, 0] = total[0:2]
        wide[b, 1] = total[2:4]

    for g, a, k in far:
        px, py, peer = ahead(g, a, k)
        pc = c if k == 0 else other
        pu, pv = py + pc * (px - py), px + pc * (py - px)
        push(
            wide.at[pu, lax.rem(pv, 2)],
            got.at[g * group + a * NC + k],
            peer,
            score_send,
            score_recv,
        )
    got[0] = wide[u, lax.rem(v, 2)]

    owner, slot_of = tile // tiles, tile % tiles
    dx, dy, dc = shift(owner)
    source = ((dy - dx) & (NY - 1)) * (NX * NC) + dx * NC + dc
    upper_half = lax.broadcasted_iota(I32, cand.shape, 0) < cand.shape[0] // 2
    turn = lax.rem(LANES - (c * (NX // 2) + v // 2) * tiles, LANES)

    arrived(got.at[pl.ds(0, n - 1)], score_recv)
    tables = [pltpu.roll(got[:, i, :], turn, 1).T for i in range(2)]
    score = jnp.zeros(cand.shape, F32)
    for s in range(tiles):
        table = jnp.where(upper_half, tables[0][s : s + 1, :], tables[1][s : s + 1, :])
        value = jnp.take_along_axis(table, source, axis=1)
        score = jnp.where(slot_of == s, value, score)
    out_ref[...] = score

    arrived(req.at[pl.ds(0, NX - 1)], rx_send)
    arrived(asked.at[pl.ds(0, NY * NC - 1)], ry_send)
    arrived(sent.at[pl.ds(0, (n - 1) * CAP)], row_send)
    arrived(qb.at[0, 0, pl.ds(0, (NX - 1) * nq)], qx_send)
    arrived(qb.at[pl.ds(0, n_up), 0], qup_send)
    arrived(qb.at[pl.ds(0, n_down), 0], qdn_send)
    arrived(qb.at[pl.ds(0, NY), 0], qc_send)
    arrived(head_out, head_send)
    arrived(got.at[pl.ds(0, n - 1)], score_send)


def per_device(
    queries,
    candidates,
    centroids,
    bucket_weights,
    centroid_shard,
    centroid_row,
    residual_codes,
    tile_count,
    last_fill,
):
    n = NX * NY * NC
    tok, dim = residual_codes.shape
    tiles = tok // TILE
    nq = queries.shape[0] * queries.shape[1]
    ncand = candidates.size // LANES
    npass = tile_count.shape[0] // LANES
    dma = pltpu.SemaphoreType.DMA
    vmem = pl.BlockSpec(memory_space=pltpu.VMEM)
    anywhere = pl.BlockSpec(memory_space=pl.ANY)
    score = pl.pallas_call(
        kernel,
        out_shape=jax.ShapeDtypeStruct((ncand, LANES), F32),
        in_specs=[vmem, vmem, anywhere, anywhere, vmem, vmem, vmem, vmem, vmem],
        out_specs=vmem,
        scratch_shapes=[
            pltpu.VMEM(centroids.shape, BF16),
            pltpu.VMEM(residual_codes.shape, I32),
            pltpu.VMEM((NX, NY * NC, LANES), I32),
            pltpu.VMEM((NX, NY * NC, LANES), I32),
            pltpu.VMEM((NY * NC, NX, LANES), I32),
            pltpu.VMEM((NX * NC * CAP, centroids.shape[0]), BF16),
            pltpu.VMEM((n * CAP, dim), BF16),
            pltpu.VMEM((n * CAP, dim), BF16),
            pltpu.VMEM((tok, 256), BF16),
            pltpu.VMEM((tok, LANES), F32),
            pltpu.VMEM((tok, dim), F32),
            pltpu.VMEM((tok, dim), F32),
            pltpu.VMEM((tok, dim), BF16),
            pltpu.VMEM((NY, NC, NX * nq, dim), BF16),
            pltpu.VMEM((tiles + 8, n * nq), F32),
            pltpu.VMEM((2, n * nq), F32),
            pltpu.VMEM((2, n * nq), F32),
            pltpu.VMEM((NY, 2, 2, LANES), F32),
            pltpu.VMEM((n, 2, LANES), F32),
            pltpu.VMEM((npass, LANES), I32),
            pltpu.VMEM((tiles, LANES), F32),
            pltpu.VMEM((tiles, LANES), F32),
            pltpu.VMEM((tiles, LANES), F32),
            dma((2,)),
            *[dma] * 5,
            dma((NY,)),
            dma,
            dma,
            dma,
            dma((NY // 2,)),
            dma,
            dma((NY // 2,)),
            *[dma] * 6,
        ],
        compiler_params=pltpu.CompilerParams(collective_id=0, has_side_effects=True),
    )(
        centroid_shard.reshape(tiles, TILE),
        centroid_row.reshape(tiles, TILE),
        centroids,
        residual_codes,
        bucket_weights,
        tile_count.reshape(npass, LANES),
        last_fill.reshape(npass, LANES),
        queries.reshape(nq, dim),
        candidates.reshape(ncand, LANES),
    )
    return score.reshape(candidates.shape)


def solution(mesh):
    both = ("groups", "psg")
    return jax.shard_map(
        per_device,
        mesh=mesh,
        in_specs=(
            P(both, None, None),
            P(both, None),
            P("psg", None),
            P(),
            P("psg", None),
            P("psg"),
            P("psg", None),
            P(),
            P(),
        ),
        out_specs=P(both, None),
        check_vma=False,
    )
```

```python
import functools

import jax
import jax.numpy as jnp
from jax import lax
from jax.experimental import pallas as pl
from jax.experimental.pallas import tpu as pltpu
from jax.sharding import PartitionSpec as P

MESH = pl.DeviceIdType.MESH
TILE = 128
LANES = 128
NX, NY, NC = 8, 8, 2
CAP = 32
EPS = 1e-06
F32, BF16, I32 = jnp.float32, jnp.bfloat16, jnp.int32


def dot(a, b, ca=1, cb=0):
    return lax.dot_general(a, b, (((ca,), (cb,)), ((), ())), preferred_element_type=F32)


def kernel(
    owner_ref,
    row_ref,
    cent_hbm,
    code_hbm,
    bw_ref,
    count_ref,
    last_ref,
    query_ref,
    cand_ref,
    out_ref,
    cent,
    code,
    req,
    mid_req,
    asked,
    onehot,
    sent,
    fetched,
    low,
    high,
    res,
    acc,
    emb,
    qb,
    tm,
    head_out,
    head_in,
    wide,
    got,
    starts,
    fills,
    join1,
    join2,
    load_sem,
    rx_send,
    rx_recv,
    ry_send,
    ry_recv,
    row_send,
    row_recv,
    qx_send,
    qx_recv,
    qup_send,
    qup_recv,
    qdn_send,
    qdn_recv,
    qc_send,
    qc_recv,
    head_send,
    head_recv,
    score_send,
    score_recv,
):
    n = NX * NY * NC
    tiles = owner_ref.shape[0]
    npass = count_ref.shape[0]
    me = lax.axis_index("psg")
    x = me // (NY * NC)
    y = lax.rem(me // NC, NY)
    c = lax.rem(me, NC)
    other = 1 - c

    def index(px, py, pc):
        return (px * NY + py) * NC + pc

    def ahead(g, a, k):
        px, py = lax.rem(x + a, NX), lax.rem(y + a + g, NY)
        return px, py, index(px, py, c if k == 0 else other)

    def shift(device):
        dx = (x - device // (NY * NC)) & (NX - 1)
        dy = (y - (device // NC) % NY) & (NY - 1)
        dc = (c - device) & (NC - 1)
        return dx, dy, dc

    def push(src, dst, where, send, recv):
        pltpu.make_async_remote_copy(
            src_ref=src,
            dst_ref=dst,
            send_sem=send,
            recv_sem=recv,
            device_id={"psg": where},
            device_id_type=MESH,
        ).start()

    def arrived(ref, sem):
        pltpu.make_async_copy(ref, ref, sem).wait()

    def at_uv(u, v):
        return (1 - c) * index(v, u, 0) + c * index(u, v, 1)

    u, v = y + c * (x - y), x + c * (y - x)

    pairs = [(a, k) for a in range(NX) for k in range(NC)]
    far = sorted(
        [(g, a, k) for g in range(NY) for a, k in pairs if (g, a, k) != (0, 0, 0)],
        key=lambda p: -min(p[1], NX - p[1]) - min((p[0] + p[1]) % NY, -(p[0] + p[1]) % NY),
    )
    group = NX * NC
    gslots = group * CAP

    barrier = pltpu.get_barrier_semaphore()
    greeted = [index(lax.rem(x + d, NX), y, c) for d in range(1, NX)]
    greeted += [
        index(x, lax.rem(y + d, NY), c if k == 0 else other)
        for d in range(NY)
        for k in range(NC)
        if (d, k) != (0, 0)
    ]
    for peer in greeted:
        pl.semaphore_signal(barrier, inc=1, device_id={"psg": peer}, device_id_type=MESH)
    cent_copy = pltpu.make_async_copy(cent_hbm, cent, load_sem.at[0])
    cent_copy.start()
    code_copy = pltpu.make_async_copy(code_hbm, code, load_sem.at[1])
    code_copy.start()

    sub = lax.broadcasted_iota(I32, (LANES, LANES), 0)
    lane = lax.broadcasted_iota(I32, (LANES, LANES), 1)
    upper = (sub <= lane).astype(BF16)
    ones = jnp.ones((LANES, LANES), BF16)
    dx, dy, dc = shift(owner_ref[...])
    rel = (dx * NY + dy) * NC + dc
    turn_of = ((dy - dx) & (NY - 1)) * (NX * NC) + dx * NC + dc
    crow = row_ref[...]
    members = [sub == rel[t : t + 1, :] for t in range(tiles)]
    flags = [m.astype(BF16) for m in members]
    running = dot(jnp.concatenate(flags, axis=0), jnp.concatenate([upper, ones], axis=1))
    carry = jnp.zeros((LANES, LANES), F32)
    slots, lows, highs = [], [], []
    for t in range(tiles):
        part = running[t * LANES : (t + 1) * LANES, :]
        count = jnp.where(members[t], part[:, :LANES] + carry, 0.0)
        carry = carry + part[:, LANES:]
        rank = jnp.sum(count, axis=0, keepdims=True).astype(I32) - 1
        slots.append(turn_of[t : t + 1, :] * CAP + rank)
        place = sub == rank
        tok = crow[t : t + 1, :]
        lows.append(jnp.where(place, (tok & 255).astype(F32), 0.0).astype(BF16))
        highs.append(jnp.where(place, (tok >> 8).astype(F32), 0.0).astype(BF16))
    values = jnp.concatenate(
        [jnp.concatenate(lows, axis=1), jnp.concatenate(highs, axis=1)], axis=0
    )
    summed = dot(jnp.concatenate(flags, axis=1), values, 1, 1)
    low_sum, high_sum = summed[:, :LANES], summed[:, LANES:]
    asking = (low_sum + 256.0 * high_sum).astype(I32)
    req[...] = asking.reshape(NX, NY * NC, LANES)

    pl.semaphore_wait(barrier, len(greeted))

    for a in range(1, NX):
        where = index(lax.rem(x + NX - a, NX), y, c)
        push(req.at[a], mid_req.at[a], where, rx_send, rx_recv)
    mid_req[0] = req[0]

    nq = query_ref.shape[0]
    own_block = qb.at[u, c, pl.ds(pl.multiple_of(v * nq, nq), nq)]
    for a in range(1, NX):
        push(query_ref, own_block, at_uv(u, lax.rem(v + a, NX)), qx_send, qx_recv)
    qb[u, c, pl.ds(pl.multiple_of(v * nq, nq), nq), :] = query_ref[...]

    arrived(mid_req.at[pl.ds(0, NX - 1)], rx_recv)
    for j in range(1, NY * NC):
        d, k = j // NC, j % NC
        where = index(x, lax.rem(y + NY - d, NY), c if k == 0 else other)
        push(mid_req.at[:, j], asked.at[j], where, ry_send, ry_recv)
    asked[0] = mid_req[:, 0, :]

    up = at_uv(lax.rem(u + 1, NY), v)
    down = at_uv(lax.rem(u + NY - 1, NY), v)
    across = index(x, y, other)
    n_up, n_down = NY - 1 - NY // 2, NY // 2

    def pass_on(block, where, send, recv):
        push(qb.at[block, c], qb.at[block, c], where, send, recv)

    arrived(qb.at[u, c, pl.ds(0, (NX - 1) * nq)], qx_recv)
    pass_on(u, up, qup_send, qup_recv.at[0])
    pass_on(u, down, qdn_send, qdn_recv.at[0])
    pass_on(u, across, qc_send, qc_recv)

    cent_copy.wait()
    half_lane = lax.broadcasted_iota(I32, (CAP, cent.shape[0]), 1).astype(F32)

    def ring(s):
        block = lax.rem(u + s, NY)
        arrived(qb.at[block, c], qdn_recv.at[s - 1])
        if s < n_down:
            pass_on(block, down, qdn_send, qdn_recv.at[s])
        pass_on(block, across, qc_send, qc_recv)
        if s <= n_up:
            block = lax.rem(u + NY - s, NY)
            arrived(qb.at[block, c], qup_recv.at[s - 1])
            if s < n_up:
                pass_on(block, up, qup_send, qup_recv.at[s])
            pass_on(block, across, qc_send, qc_recv)

    ring(1)
    arrived(asked.at[pl.ds(0, NY * NC - 1)], ry_recv)
    for g in range(NY):
        wanted = jnp.concatenate(
            [asked[(a + g) % NY * NC + k, a : a + 1, :] for a, k in pairs], axis=0
        )
        wanted = wanted.astype(F32).T
        for j in range(group):
            onehot[pl.ds(j * CAP, CAP), :] = (wanted[:CAP, j : j + 1] == half_lane).astype(BF16)
        found = dot(onehot[...], cent[...]).astype(BF16)
        sent[pl.ds(g * gslots, gslots), :] = found
        if g == 0:
            fetched[pl.ds(0, CAP), :] = found[:CAP]
        for a, k in pairs:
            if (g, a, k) != (0, 0, 0):
                at = pl.ds((g * group + a * NC + k) * CAP, CAP)
                pltpu.make_async_remote_copy(
                    src_ref=sent.at[at],
                    dst_ref=fetched.at[at],
                    send_sem=row_send,
                    recv_sem=row_recv.at[g],
                    device_id={"psg": ahead(g, a, k)[2]},
                    device_id_type=MESH,
                ).start()
        if g == 3:
            ring(2)

    ring(3)
    slot = jnp.concatenate(slots, axis=0)
    pad = jnp.zeros((LANES - tiles, LANES), F32)
    low_t = jnp.concatenate([(slot & 255).astype(F32), pad], axis=0).T
    high_t = jnp.concatenate([(slot >> 8).astype(F32), pad], axis=0).T
    wide_lane = lax.broadcasted_iota(I32, (LANES, 256), 1).astype(F32)
    for t in range(tiles):
        at = pl.ds(t * TILE, TILE)
        low[at, :] = (low_t[:, t : t + 1] == wide_lane).astype(BF16)
        high[at, :] = jnp.broadcast_to(high_t[:, t : t + 1], (TILE, LANES))

    counts = count_ref[...].astype(F32)
    sums = dot(counts.astype(BF16), upper)
    before = jnp.zeros((1, 1), F32)
    rows = []
    for r in range(npass):
        rows.append(sums[r : r + 1, :] + before)
        before = before + sums[r : r + 1, LANES - 1 : LANES]
    ends = jnp.concatenate(rows, axis=0)
    starts[...] = (ends - counts).astype(I32)
    final = ends.astype(I32) - 1
    last = last_ref[...].astype(F32)
    fill_rows, end_rows = [], []
    for t in range(tiles + 1):
        hit = final == me * tiles + t
        fill_rows.append(jnp.sum(jnp.where(hit, last, 0.0), axis=0, keepdims=True))
        end_rows.append(jnp.sum(jnp.where(hit, 1.0, 0.0), axis=0, keepdims=True))
    fill = jnp.sum(jnp.concatenate(fill_rows, axis=0), axis=1, keepdims=True)
    ending = jnp.sum(jnp.concatenate(end_rows, axis=0), axis=1, keepdims=True)
    fills[...] = jnp.broadcast_to(jnp.where(ending > 0, fill, float(TILE))[:tiles], (tiles, LANES))
    goes = ending == 0
    join1[...] = jnp.broadcast_to(goes[:tiles].astype(F32), (tiles, LANES))
    join2[...] = jnp.broadcast_to(
        goes[:tiles].astype(F32) * goes[1 : tiles + 1].astype(F32), (tiles, LANES)
    )

    code_copy.wait()

    @pl.loop(0, tiles, unroll=4)
    def _(t):
        at = pl.ds(pl.multiple_of(t * TILE, TILE), TILE)
        v = code[at, :]
        first = jnp.where(v == 0, bw_ref[0:1, :], bw_ref[1:2, :])
        second = jnp.where(v == 2, bw_ref[2:3, :], bw_ref[3:4, :])
        res[at, :] = jnp.where(v < 2, first, second)

    cuts = [
        (i, slice(j, j + LANES))
        for i in range(cand_ref.shape[0])
        for j in range(0, cand_ref.shape[1], LANES)
    ]
    cand = jnp.concatenate([cand_ref[i : i + 1, at] for i, at in cuts], axis=0)
    tile = jnp.zeros(cand.shape, I32)
    for r in range(npass):
        table = jnp.broadcast_to(starts[r : r + 1, :], cand.shape)
        value = jnp.take_along_axis(table, cand & (LANES - 1), axis=1)
        tile = jnp.where(cand >> 7 == r, value, tile)
    ring(4)

    span = 4 * TILE
    for g in range(NY):
        count = (group - 1 if g == 0 else group) * CAP
        arrived(fetched.at[pl.ds(0, count)], row_recv.at[g])
        base = g * gslots
        both = jnp.concatenate(
            [fetched[pl.ds(base, 256), :], fetched[pl.ds(base + 256, 256), :]], axis=1
        )

        @pl.loop(0, tiles * TILE // span, unroll=4)
        def _(i):
            at = pl.ds(pl.multiple_of(i * span, span), span)
            picked = dot(low[at, :], both)
            which = high[at, :]
            keep = 0.0 if g == 0 else acc[at, :]
            keep = jnp.where(which == float(2 * g + 1), picked[:, LANES:], keep)
            acc[at, :] = jnp.where(which == float(2 * g), picked[:, :LANES], keep)

    @pl.loop(0, tiles, unroll=8)
    def _(t):
        at = pl.ds(pl.multiple_of(t * TILE, TILE), TILE)
        summed = acc[at, :] + res[at, :]
        scale = lax.rsqrt(jnp.sum(summed * summed, axis=1, keepdims=True) + EPS)
        unit = summed * scale
        unit = jnp.where(sub.astype(F32) < fills[pl.ds(t, 1), :], unit, unit[0:1, :])
        emb[at, :] = unit.astype(BF16)

    arrived(qb.at[pl.ds(0, NY), 0], qc_recv)

    span = tiles // 2
    chunk = 256
    per = qb.shape[2] // chunk

    def maxima(half):
        @pl.loop(0, NY * NC * per, unroll=16)
        def _(i):
            part = qb[
                i // (NC * per),
                lax.rem(i // per, NC),
                pl.ds(pl.multiple_of(lax.rem(i, per) * chunk, chunk), chunk),
                :,
            ]
            at = pl.ds(pl.multiple_of(i * chunk, chunk), chunk)
            s = dot(emb[pl.ds(half * span * TILE, span * TILE), :], part, 1, 1)
            top = jnp.max(s.reshape(span, TILE, chunk), axis=1)
            tm[pl.ds(half * span, span), at] = top
            if half == 0:
                head_out[:, at] = top[0:2, :]

    maxima(0)
    pltpu.make_async_remote_copy(
        src_ref=head_out,
        dst_ref=head_in,
        send_sem=head_send,
        recv_sem=head_recv,
        device_id={"psg": lax.rem(me + n - 1, n)},
        device_id_type=MESH,
    ).start()
    maxima(1)
    arrived(head_in, head_recv)
    tm[tiles : tiles + 2, :] = head_in[...]

    width = NX * LANES
    first_join, second_join = join1[...] > 0, join2[...] > 0
    for b in range(NY):
        stack = []
        for i in range(NX):
            at = pl.ds(b * width + i * LANES, LANES)
            one = tm[0:tiles, at]
            one = jnp.maximum(one, jnp.where(first_join, tm[1 : tiles + 1, at], one))
            one = jnp.maximum(one, jnp.where(second_join, tm[2 : tiles + 2, at], one))
            stack.append(one)
        turned = jnp.concatenate(stack, axis=0).T
        total = jnp.sum(turned.reshape(4, 32, LANES), axis=1)
        wide[b, 0] = total[0:2]
        wide[b, 1] = total[2:4]

    for g, a, k in far:
        px, py, peer = ahead(g, a, k)
        pc = c if k == 0 else other
        pu, pv = py + pc * (px - py), px + pc * (py - px)
        push(
            wide.at[pu, lax.rem(pv, 2)],
            got.at[g * group + a * NC + k],
            peer,
            score_send,
            score_recv,
        )
    got[0] = wide[u, lax.rem(v, 2)]

    owner, slot_of = tile // tiles, tile % tiles
    dx, dy, dc = shift(owner)
    source = ((dy - dx) & (NY - 1)) * (NX * NC) + dx * NC + dc
    upper_half = lax.broadcasted_iota(I32, cand.shape, 0) < cand.shape[0] // 2
    turn = lax.rem(LANES - (c * (NX // 2) + v // 2) * tiles, LANES)

    arrived(got.at[pl.ds(0, n - 1)], score_recv)
    tables = [pltpu.roll(got[:, i, :], turn, 1).T for i in range(2)]
    score = jnp.zeros(cand.shape, F32)
    for s in range(tiles):
        table = jnp.where(upper_half, tables[0][s : s + 1, :], tables[1][s : s + 1, :])
        value = jnp.take_along_axis(table, source, axis=1)
        score = jnp.where(slot_of == s, value, score)
    for r, (i, at) in enumerate(cuts):
        out_ref[i : i + 1, at] = score[r : r + 1, :]

    arrived(req.at[pl.ds(0, NX - 1)], rx_send)
    arrived(asked.at[pl.ds(0, NY * NC - 1)], ry_send)
    arrived(sent.at[pl.ds(0, (n - 1) * CAP)], row_send)
    arrived(qb.at[0, 0, pl.ds(0, (NX - 1) * nq)], qx_send)
    arrived(qb.at[pl.ds(0, n_up), 0], qup_send)
    arrived(qb.at[pl.ds(0, n_down), 0], qdn_send)
    arrived(qb.at[pl.ds(0, NY), 0], qc_send)
    arrived(head_out, head_send)
    arrived(got.at[pl.ds(0, n - 1)], score_send)


def per_device(
    queries,
    candidates,
    centroids,
    bucket_weights,
    centroid_shard,
    centroid_row,
    residual_codes,
    tile_count,
    last_fill,
):
    n = NX * NY * NC
    tok, dim = residual_codes.shape
    tiles = tok // TILE
    nq = queries.shape[0] * queries.shape[1]
    npass = tile_count.shape[0] // LANES
    dma = pltpu.SemaphoreType.DMA
    vmem = pl.BlockSpec(memory_space=pltpu.VMEM)
    anywhere = pl.BlockSpec(memory_space=pl.ANY)
    return pl.pallas_call(
        kernel,
        out_shape=jax.ShapeDtypeStruct(candidates.shape, F32),
        in_specs=[vmem, vmem, anywhere, anywhere, vmem, vmem, vmem, vmem, vmem],
        out_specs=vmem,
        scratch_shapes=[
            pltpu.VMEM(centroids.shape, BF16),
            pltpu.VMEM(residual_codes.shape, I32),
            pltpu.VMEM((NX, NY * NC, LANES), I32),
            pltpu.VMEM((NX, NY * NC, LANES), I32),
            pltpu.VMEM((NY * NC, NX, LANES), I32),
            pltpu.VMEM((NX * NC * CAP, centroids.shape[0]), BF16),
            pltpu.VMEM((n * CAP, dim), BF16),
            pltpu.VMEM((n * CAP, dim), BF16),
            pltpu.VMEM((tok, 256), BF16),
            pltpu.VMEM((tok, LANES), F32),
            pltpu.VMEM((tok, dim), F32),
            pltpu.VMEM((tok, dim), F32),
            pltpu.VMEM((tok, dim), BF16),
            pltpu.VMEM((NY, NC, NX * nq, dim), BF16),
            pltpu.VMEM((tiles + 8, n * nq), F32),
            pltpu.VMEM((2, n * nq), F32),
            pltpu.VMEM((2, n * nq), F32),
            pltpu.VMEM((NY, 2, 2, LANES), F32),
            pltpu.VMEM((n, 2, LANES), F32),
            pltpu.VMEM((npass, LANES), I32),
            pltpu.VMEM((tiles, LANES), F32),
            pltpu.VMEM((tiles, LANES), F32),
            pltpu.VMEM((tiles, LANES), F32),
            dma((2,)),
            *[dma] * 5,
            dma((NY,)),
            dma,
            dma,
            dma,
            dma((NY // 2,)),
            dma,
            dma((NY // 2,)),
            *[dma] * 6,
        ],
        compiler_params=pltpu.CompilerParams(collective_id=0, has_side_effects=True),
    )(
        centroid_shard.reshape(tiles, TILE),
        centroid_row.reshape(tiles, TILE),
        centroids,
        residual_codes,
        bucket_weights,
        tile_count.reshape(npass, LANES),
        last_fill.reshape(npass, LANES),
        queries.reshape(nq, dim),
        candidates,
    )


def solution(mesh):
    both = ("groups", "psg")
    return jax.shard_map(
        per_device,
        mesh=mesh,
        in_specs=(
            P(both, None, None),
            P(both, None),
            P("psg", None),
            P(),
            P("psg", None),
            P("psg"),
            P("psg", None),
            P(),
            P(),
        ),
        out_specs=P(both, None),
        check_vma=False,
    )
```
